512 devices in a mesh: dp: 64 (over z, y), tensor: 8 (over x, core).
Axes of the slice: x: 4, y: 8, z: 8, core: 2. Of those that a mesh axis runs over, the one named last changes fastest.
Arguments:
- gradient: bfloat16 [64, 512, 8192], P('dp', 'tensor'), may hold values from -110 to 110
- momentum: bfloat16 [64, 512, 8192], P('dp', 'tensor'), may hold values from -6 to 6
- indices: int32 [64, 8, 128, 32], P('dp', 'tensor'), may hold values from 0 to 4095, all different within a row
Outputs:
- new_momentum: bfloat16 [64, 512, 8192], P('dp', 'tensor')
- update: bfloat16 [512, 8192], P('tensor')
The draws below stay inside these ranges and needn't reach their ends.
Inputs may be any that keep to these rules, and one draw needn't show every extreme that they name: The 32 indices of one span of one replica are distinct; index a * 64 + b names row frequency a and column frequency b.
All inputs are finite; a program needn't handle non-finite values.
Results may differ from the reference program's by a relative error of at most 0.0049.
Values may be sent and summed in bfloat16 or wider, within the bound.
A program may use at most 64 MiB of HBM per device.

```python
import jax
import jax.numpy as jnp
from jax import lax

D = 8192
BLOCK = 64
TOPK = 32
ROWS = 512
REPLICAS = 64


def draw_gradient(key, part):
    keys = jax.random.split(key, 3)
    own = jnp.clip(jax.random.normal(keys[0], (REPLICAS, ROWS, D), jnp.float32), -4.0, 4.0)
    position = jnp.arange(ROWS, dtype=jnp.float32) / ROWS
    rough_rows = jax.random.uniform(keys[1], (ROWS,), jnp.float32, 0.5, 2.0)
    rough_cols = jax.random.uniform(keys[2], (D,), jnp.float32, 0.5, 2.0)
    ramp = 10.0 ** (position - 0.5) * rough_rows
    return (own * ramp[None, :, None] * rough_cols[None, None, :]).astype(jnp.bfloat16)


def levels(rng, extent, shards, least, largest):
    gain, own = 1.0, jax.random.fold_in(rng, 6)
    for dim, parts in shards:
        heights = jnp.exp(jax.random.uniform(jax.random.fold_in(own, dim), (parts,), jnp.float32, least / len(shards), largest / len(shards)))
        gain = gain * jnp.repeat(heights, extent[dim] // parts).reshape([-1 if axis == dim else 1 for axis in range(len(extent))])
    return gain


def choose_distinct(key, rows, amount, top, lift):
    sequence = jax.random.permutation(jax.random.fold_in(key, 1), amount)
    pull = sequence
    for power in range(3):
        pull = pull * pull // amount
    pull = pull * lift // amount
    lots = jax.random.randint(jax.random.fold_in(key, 2), (rows, amount), 0, 4096) + pull
    sure = jax.random.permutation(jax.random.fold_in(key, 3), rows)[jnp.arange(amount) % rows]
    lots = jnp.where(jnp.arange(rows)[:, None] == sure[None, :], 1 << 14, lots)
    priority = lots * amount + jnp.arange(amount)
    return lax.top_k(priority.astype(jnp.int32), top)[1].astype(jnp.int32)


def noise(rng, extent, width, limit, shards=(), kind=jnp.bfloat16):
    loudness = levels(rng, extent, shards, -0.22, 0.18) if shards else 1.0
    array = jax.random.normal(rng, extent, jnp.float32) * width * loudness
    return jnp.minimum(jnp.maximum(array, -limit), limit).astype(kind)


def setup_inputs(seed: int = 0) -> dict:
    arg_keys = jax.random.split(jax.random.key(seed), 4)
    gradient = draw_gradient(jax.random.fold_in(arg_keys[3], 71), 0)
    momentum = noise(arg_keys[1], (REPLICAS, ROWS, D), 1.0, 6.0, ((0, 64), (1, 8)))
    indices = choose_distinct(arg_keys[2], REPLICAS * (ROWS // BLOCK) * (D // BLOCK), BLOCK * BLOCK, TOPK, 0).reshape((REPLICAS, ROWS // BLOCK, D // BLOCK, TOPK))
    return dict(gradient=gradient, momentum=momentum, indices=indices)


EPSILON = 1e-06
DECAY = 0.999

def dct_basis(block_edge):
    frequency = jnp.arange(block_edge, dtype=jnp.float32)[:, None]
    position = jnp.arange(block_edge, dtype=jnp.float32)[None, :]
    waves = jnp.cos(jnp.pi * (2.0 * position + 1.0) * frequency / (2.0 * block_edge))
    weights = jnp.where(frequency == 0.0, jnp.sqrt(1.0 / block_edge), jnp.sqrt(2.0 / block_edge))
    return waves * weights

def reference(gradient, momentum, indices):
    cosines = dct_basis(BLOCK)
    row_blocks = ROWS // BLOCK
    col_blocks = D // BLOCK
    precise = lax.Precision.HIGHEST
    block_rows = jnp.arange(row_blocks, dtype=jnp.int32)[:, None, None]
    block_cols = jnp.arange(col_blocks, dtype=jnp.int32)[None, :, None]

    def to_spans(slab):
        return slab.reshape(row_blocks, BLOCK, col_blocks, BLOCK).transpose(0, 2, 1, 3)

    def from_spans(blocks):
        return blocks.transpose(0, 2, 1, 3).reshape(ROWS, D)

    def compress(operands):
        grad_slab, moment_slab, chosen = operands
        renewed = DECAY * moment_slab.astype(jnp.float32) + grad_slab.astype(jnp.float32)
        spectrum = jnp.einsum('ka,pqab,lb->pqkl', cosines, to_spans(renewed), cosines, precision=precise)
        flattened = spectrum.reshape(row_blocks, col_blocks, BLOCK * BLOCK)
        picked = jnp.take_along_axis(flattened, chosen, axis=2)
        marker = jnp.zeros_like(flattened).at[block_rows, block_cols, chosen].set(1.0)
        retained = (flattened * marker).reshape(row_blocks, col_blocks, BLOCK, BLOCK)
        restored = jnp.einsum('ka,pqkl,lb->pqab', cosines, retained, cosines, precision=precise)
        return ((renewed - from_spans(restored)).astype(jnp.bfloat16), picked.astype(jnp.bfloat16))
    new_momentum, values = lax.map(compress, (gradient, momentum, indices))

    def absorb(running, operands):
        shipped, chosen = operands
        return (running.at[block_rows, block_cols, chosen].add(shipped.astype(jnp.float32)), None)
    start_sum = jnp.zeros((row_blocks, col_blocks, BLOCK * BLOCK), jnp.float32)
    combined, unused = lax.scan(absorb, start_sum, (values, indices))
    combined = combined.reshape(row_blocks, col_blocks, BLOCK, BLOCK)
    decoded = from_spans(jnp.einsum('ka,pqkl,lb->pqab', cosines, combined, cosines, precision=precise))
    spread = jnp.sqrt(jnp.mean(decoded * decoded) + EPSILON)
    update = (decoded / spread).astype(jnp.bfloat16)
    return (new_momentum, update)
```

```python
import functools

import jax
import jax.numpy as jnp
import numpy as np
from jax import lax
from jax.experimental import pallas as pl
from jax.experimental.pallas import tpu as pltpu
from jax.sharding import PartitionSpec as P

MESH = pl.DeviceIdType.MESH
BLOCK = 64
TOPK = 32
CHUNK = 256
RING = 8
GROUP = 4
EPSILON = 1e-06
DECAY = 0.999
F32 = jnp.float32
BF16 = jnp.bfloat16


def basis():
    frequency = np.arange(BLOCK, dtype=np.float64)[:, None]
    position = np.arange(BLOCK, dtype=np.float64)[None, :]
    waves = np.cos(np.pi * (2.0 * position + 1.0) * frequency / (2.0 * BLOCK))
    return waves * np.where(frequency == 0.0, np.sqrt(1.0 / BLOCK), np.sqrt(2.0 / BLOCK))


def halves(array):
    array = array.astype(np.float32)
    high = array.astype(BF16)
    low = (array - high.astype(np.float32)).astype(BF16)
    return high, low


def right_constants(matrix):
    return np.stack([np.kron(np.eye(4), half.astype(np.float32)).astype(BF16) for half in halves(matrix)])


def left_constants(matrix):
    high, low = halves(matrix)
    return np.concatenate([high, high, low, low], axis=1)


def dot(a, b):
    return jnp.dot(a, b, preferred_element_type=F32)


def dot_nt(a, b):
    return lax.dot_general(a, b, (((1,), (1,)), ((), ())), preferred_element_type=F32)


def split(x):
    high = x.astype(BF16)
    return high, (x - high.astype(F32)).astype(BF16)


def left(constants, y):
    high, low = split(y)
    return dot(constants, jnp.concatenate([high, low, high, low], axis=0))


def right(x, high_constants, low_constants):
    high, low = split(x)
    return dot(high, high_constants) + dot(low, high_constants) + dot(high, low_constants)


def iota(shape, dim):
    return lax.broadcasted_iota(jnp.int32, shape, dim)


def kernel(
    total_count,
    g_hbm,
    m_hbm,
    idx_ref,
    fwd_right,
    inv_right,
    fwd_left,
    inv_left,
    nm_hbm,
    up_hbm,
    g_ref,
    m_ref,
    nm_ref,
    up_ref,
    s_ref,
    ob_ref,
    oa_ref,
    turned_ref,
    il_ref,
    msg_ref,
    recv_ref,
    land_ref,
    ex_ref,
    ey_ref,
    ez_ref,
    in_sem,
    out_sem,
    msg_send,
    msg_recv,
    land_send,
    land_recv,
    e_send,
    e_recv,
):
    me = lax.axis_index("dp")
    tensor = lax.axis_index("tensor")
    z, y = me // RING, lax.rem(me, RING)
    replicas = RING * RING
    chunks = s_ref.shape[0]
    groups = chunks // GROUP
    wide = GROUP * CHUNK

    def group_columns(i):
        return pl.ds(pl.multiple_of(i * wide, wide), wide)

    def load(i, which):
        hbm, ref = ((g_hbm, g_ref), (m_hbm, m_ref))[which]
        return pltpu.make_async_copy(
            hbm.at[0, :, group_columns(i)], ref.at[:, group_columns(i)], in_sem.at[which, i]
        )

    for i in range(groups):
        load(i, 0).start()
        load(i, 1).start()

    barrier = pltpu.get_barrier_semaphore()

    def greet_dp(k, carry):
        pl.semaphore_signal(barrier, inc=1, device_id={"dp": lax.rem(me + k, replicas)}, device_id_type=MESH)
        return carry

    def greet_tensor(k, carry):
        pl.semaphore_signal(barrier, inc=1, device_id={"tensor": lax.rem(tensor + k, RING)}, device_id_type=MESH)
        return carry

    lax.fori_loop(1, replicas, greet_dp, 0)
    lax.fori_loop(1, RING, greet_tensor, 0)

    turned_ref[...] = jnp.transpose(idx_ref[...])
    il_ref[...] = jnp.concatenate(
        [turned_ref[pl.ds(k, chunks, stride=4), :] for k in range(4)], axis=1
    )
    lane_span = iota((1, 128), 1) // TOPK

    def renewed(c):
        columns = pl.ds(pl.multiple_of(c * CHUNK, CHUNK), CHUNK)
        return DECAY * m_ref[:, columns].astype(F32) + g_ref[:, columns].astype(F32)

    def compress(i, carry):
        load(i, 0).wait()
        load(i, 1).wait()
        pieces = [split(renewed(i * GROUP + c)) for c in range(GROUP)]
        high = jnp.concatenate([p[0] for p in pieces], axis=0)
        low = jnp.concatenate([p[1] for p in pieces], axis=0)
        half = dot(high, fwd_right[0]) + dot(low, fwd_right[0]) + dot(high, fwd_right[1])
        for c in range(GROUP):
            chunk = i * GROUP + c
            spectrum = left(fwd_left[...], half[c * BLOCK : (c + 1) * BLOCK])
            s_ref[chunk] = spectrum
            ids = il_ref[pl.ds(chunk, 1), :]
            row_hit = iota((BLOCK, 128), 0) == ids // BLOCK
            col_hit = iota((CHUNK, 128), 0) == lax.rem(ids, BLOCK) + BLOCK * lane_span
            col_ones = jnp.where(col_hit, 1.0, 0.0).astype(BF16)
            ob_ref[chunk] = col_ones
            oa_ref[chunk] = jnp.where(row_hit, 1.0, 0.0).astype(BF16)
            by_column = dot(spectrum.astype(BF16), col_ones)
            msg_ref[chunk, 0:1, :] = jnp.sum(jnp.where(row_hit, by_column, 0.0), axis=0, keepdims=True)
            msg_ref[chunk, 1:2, :] = ids.astype(F32)
        return carry

    lax.fori_loop(0, groups, compress, 0)

    pl.semaphore_wait(barrier, replicas - 1 + RING - 1)

    def send_values(k, carry):
        peer = lax.rem(me + k, replicas)
        pltpu.make_async_remote_copy(
            src_ref=msg_ref.at[peer // 2],
            dst_ref=recv_ref.at[me],
            send_sem=msg_send,
            recv_sem=msg_recv,
            device_id={"dp": peer},
            device_id_type=MESH,
        ).start()
        return carry

    lax.fori_loop(1, replicas, send_values, 0)

    def store(i):
        return pltpu.make_async_copy(
            nm_ref.at[:, group_columns(i)], nm_hbm.at[0, :, group_columns(i)], out_sem.at[0, i]
        )

    def remove(i, carry):
        rows = []
        for c in range(GROUP):
            chunk = i * GROUP + c
            marker = dot_nt(oa_ref[chunk], ob_ref[chunk])
            rows.append(split(left(inv_left[...], s_ref[chunk] * marker)))
        high = jnp.concatenate([r[0] for r in rows], axis=0)
        low = jnp.concatenate([r[1] for r in rows], axis=0)
        restored = dot(high, inv_right[0]) + dot(low, inv_right[0]) + dot(high, inv_right[1])
        for c in range(GROUP):
            chunk = i * GROUP + c
            columns = pl.ds(pl.multiple_of(chunk * CHUNK, CHUNK), CHUNK)
            nm_ref[:, columns] = (renewed(chunk) - restored[c * BLOCK : (c + 1) * BLOCK]).astype(BF16)
        store(i).start()
        return carry

    lax.fori_loop(0, groups, remove, 0)

    others = recv_ref.at[pl.ds(0, replicas - 1)]
    pltpu.make_async_copy(others, others, msg_recv).wait()
    recv_ref[me] = msg_ref[me // 2]

    odd = lax.rem(me, 2)
    lane = iota((replicas // 2, 128), 1)

    def mine(array):
        array = jnp.where(odd == 0, array, pltpu.roll(array, 64, 1))
        return jnp.where(lane < 64, array[: replicas // 2], pltpu.roll(array[replicas // 2 :], 64, 1))

    got_values = mine(recv_ref[:, 0, :])
    got_ids = mine(recv_ref[:, 1, :]).astype(jnp.int32)
    got_rows = got_ids // BLOCK
    got_cols = lax.rem(got_ids, BLOCK) + BLOCK * lax.rem(lane // TOPK, 2)
    combined = jnp.zeros((BLOCK, 128), F32)
    for r in range(0, replicas // 2, 2):
        rows, cols = [], []
        for k in (r, r + 1):
            rows.append(
                jnp.where(iota((BLOCK, 128), 0) == got_rows[k : k + 1], got_values[k : k + 1], 0.0).astype(BF16)
            )
            cols.append(jnp.where(iota((128, 128), 0) == got_cols[k : k + 1], 1.0, 0.0).astype(BF16))
        combined += dot_nt(jnp.concatenate(rows, axis=1), jnp.concatenate(cols, axis=1))
    decoded = left(inv_left[...], right(combined, inv_right[0, :128, :128], inv_right[1, :128, :128]))
    rounded = decoded.astype(BF16)
    half_rows = BLOCK // 2
    land_ref[0, me] = rounded[:half_rows]
    land_ref[1, me] = rounded[half_rows:]

    energy_refs = (ex_ref, ey_ref, ez_ref)
    energy_places = (tensor, y, z)

    def energy_target(stage, place):
        if stage == 0:
            return {"tensor": place}
        return {"dp": z * RING + place if stage == 1 else place * RING + y}

    def send_energy(stage, row):
        ref, place = energy_refs[stage], energy_places[stage]
        ref[place] = row

        def send(k, carry):
            peer = lax.rem(place + k, RING)
            pltpu.make_async_remote_copy(
                src_ref=ref.at[place],
                dst_ref=ref.at[place],
                send_sem=e_send.at[stage],
                recv_sem=e_recv.at[stage],
                device_id=energy_target(stage, peer),
                device_id_type=MESH,
            ).start()
            return carry

        lax.fori_loop(1, RING, send, 0)

    def take_energy(stage):
        ref = energy_refs[stage]
        rest = ref.at[pl.ds(0, RING - 1)]
        pltpu.make_async_copy(rest, rest, e_recv.at[stage]).wait()
        pltpu.make_async_copy(rest, rest, e_send.at[stage]).wait()
        row = ref[0]
        for k in range(1, RING):
            row = row + ref[k]
        return row

    send_energy(0, jnp.sum(decoded * decoded, axis=0, keepdims=True))

    along = ((y, z), (z, y))

    def place_of(h, a, b):
        a, b = lax.rem(a + 2 * RING, RING), lax.rem(b + 2 * RING, RING)
        return b * RING + a if h == 0 else a * RING + b

    def send_item(h, item, target):
        pltpu.make_async_remote_copy(
            src_ref=land_ref.at[h, item],
            dst_ref=land_ref.at[h, item],
            send_sem=land_send.at[h],
            recv_sem=land_recv.at[h, item],
            device_id={"dp": target},
            device_id_type=MESH,
        ).start()

    def wait_item(h, item):
        ref = land_ref.at[h, item]
        pltpu.make_async_copy(ref, ref, land_recv.at[h, item]).wait()

    def nearest(i):
        return ((i + 1) // 2) * (2 * lax.rem(i, 2) - 1)

    def first_sends(i, carry):
        for h in range(2):
            a, b = along[h]
            send_item(h, me, place_of(h, a + nearest(RING - i), b))
        return carry

    lax.fori_loop(1, RING, first_sends, 0)

    def spread(h, item):
        a, b = along[h]
        for step in (2, -2, 1, -1):
            send_item(h, item, place_of(h, a, b + step))

    for h in range(2):
        spread(h, me)

    def second_sends(i, carry):
        for h in range(2):
            a, b = along[h]
            item = place_of(h, a + nearest(i), b)
            wait_item(h, item)
            spread(h, item)
        return carry

    lax.fori_loop(1, 4, second_sends, 0)
    send_energy(1, take_energy(0))
    lax.fori_loop(4, RING, second_sends, 0)

    def third_sends(i, carry):
        for h in range(2):
            a, b = along[h]
            other = a + jnp.where(i == 0, 0, nearest(i))
            other = lax.rem(other + RING, RING)
            for step in (2, -2):
                item = place_of(h, other, b - step)
                wait_item(h, item)
                send_item(h, item, place_of(h, a, b + step // 2))
            sign = 1 - 2 * lax.rem(other, 2)
            send_item(h, place_of(h, other, b - 2 * sign), place_of(h, a, b + 2 * sign))
        return carry

    lax.fori_loop(0, 4, third_sends, 0)
    send_energy(2, take_energy(1))
    lax.fori_loop(4, RING, third_sends, 0)

    energy = jnp.sum(take_energy(2), axis=1, keepdims=True)
    scale = 1.0 / jnp.sqrt(energy / total_count + EPSILON)

    def last_waits(i, carry):
        for h in range(2):
            b = along[h][1]
            for step in (1, -1, 3, -3, 4):
                wait_item(h, place_of(h, i, b + step))
        return carry

    lax.fori_loop(0, RING, last_waits, 0)

    def put(i):
        return pltpu.make_async_copy(up_ref.at[:, group_columns(i)], up_hbm.at[:, group_columns(i)], out_sem.at[1, i])

    per_group = wide // 128

    def finish(i, carry):
        for k in range(per_group):
            item = i * per_group + k
            columns = pl.ds(pl.multiple_of(item * 128, 128), 128)
            for h in range(2):
                up_ref[h * half_rows : (h + 1) * half_rows, columns] = (
                    land_ref[h, item].astype(F32) * scale
                ).astype(BF16)
        put(i).start()
        return carry

    lax.fori_loop(0, groups, finish, 0)

    pltpu.make_async_copy(others, others, msg_send).wait()
    for h in range(2):
        rest = land_ref.at[h, pl.ds(0, replicas - 1)]
        pltpu.make_async_copy(rest, rest, land_send.at[h]).wait()
    for i in range(groups):
        store(i).wait()
        put(i).wait()


def local(total_count, gradient, momentum, indices):
    _, height, columns = gradient.shape
    chunks = columns // CHUNK
    groups = chunks // GROUP
    replicas = RING * RING
    cosines = basis()
    anywhere = pl.BlockSpec(memory_space=pl.ANY)
    vmem = pl.BlockSpec(memory_space=pltpu.VMEM)
    dma = pltpu.SemaphoreType.DMA
    return pl.pallas_call(
        functools.partial(kernel, total_count),
        out_shape=(
            jax.ShapeDtypeStruct((1, height, columns), BF16),
            jax.ShapeDtypeStruct((height, columns), BF16),
        ),
        in_specs=[anywhere, anywhere, vmem, vmem, vmem, vmem, vmem],
        out_specs=(anywhere, anywhere),
        scratch_shapes=[
            pltpu.VMEM((height, columns), BF16),
            pltpu.VMEM((height, columns), BF16),
            pltpu.VMEM((height, columns), BF16),
            pltpu.VMEM((height, columns), BF16),
            pltpu.VMEM((chunks, BLOCK, CHUNK), F32),
            pltpu.VMEM((chunks, CHUNK, 128), BF16),
            pltpu.VMEM((chunks, BLOCK, 128), BF16),
            pltpu.VMEM((chunks * 4, TOPK), jnp.int32),
            pltpu.VMEM((chunks, 128), jnp.int32),
            pltpu.VMEM((chunks, 2, 128), F32),
            pltpu.VMEM((replicas, 2, 128), F32),
            pltpu.VMEM((2, replicas, BLOCK // 2, 128), BF16),
            pltpu.VMEM((RING, 1, 128), F32),
            pltpu.VMEM((RING, 1, 128), F32),
            pltpu.VMEM((RING, 1, 128), F32),
            dma((2, groups)),
            dma((2, groups)),
            dma,
            dma,
            dma((2,)),
            dma((2, replicas)),
            dma((3,)),
            dma((3,)),
        ],
        compiler_params=pltpu.CompilerParams(collective_id=0, has_side_effects=True),
        name="demo_step",
    )(
        gradient,
        momentum,
        jnp.transpose(indices.reshape(columns // BLOCK, TOPK)),
        right_constants(cosines.T),
        right_constants(cosines),
        left_constants(cosines),
        left_constants(cosines.T),
    )


def solution(mesh):
    def whole(gradient, momentum, indices):
        rows, columns = gradient.shape[1:]
        return jax.shard_map(
            functools.partial(local, float(rows * columns)),
            mesh=mesh,
            in_specs=(P("dp", "tensor", None), P("dp", "tensor", None), P("dp", "tensor", None, None)),
            out_specs=(P("dp", "tensor", None), P("tensor", None)),
            check_vma=False,
        )(gradient, momentum, indices)

    return whole
```

```python
import functools

import jax
import jax.numpy as jnp
import numpy as np
from jax import lax
from jax.experimental import pallas as pl
from jax.experimental.pallas import tpu as pltpu
from jax.sharding import PartitionSpec as P

MESH = pl.DeviceIdType.MESH
BLOCK = 64
TOPK = 32
CHUNK = 256
RING = 8
GROUP = 8
EPSILON = 1e-06
DECAY = 0.999
F32 = jnp.float32
BF16 = jnp.bfloat16


def basis():
    frequency = np.arange(BLOCK, dtype=np.float64)[:, None]
    position = np.arange(BLOCK, dtype=np.float64)[None, :]
    waves = np.cos(np.pi * (2.0 * position + 1.0) * frequency / (2.0 * BLOCK))
    return waves * np.where(frequency == 0.0, np.sqrt(1.0 / BLOCK), np.sqrt(2.0 / BLOCK))


def halves(array):
    array = array.astype(np.float32)
    high = array.astype(BF16)
    low = (array - high.astype(np.float32)).astype(BF16)
    return high, low


def right_constants(matrix):
    return np.stack([np.kron(np.eye(4), half.astype(np.float32)).astype(BF16) for half in halves(matrix)])


def pair_constants(matrix):
    pair = np.concatenate([np.kron(np.eye(2), half.astype(np.float32)).astype(BF16) for half in halves(matrix)], axis=1)
    return np.concatenate([pair, pair], axis=0)


def entry_constants(matrix):
    return np.concatenate(
        [np.concatenate(pair, axis=1) for pair in zip(halves(DECAY * matrix), halves(matrix))], axis=0
    )


def left_constants(matrix):
    high, low = halves(matrix)
    return np.concatenate([high, high, low, low], axis=1)


def dot(a, b):
    return jnp.dot(a, b, preferred_element_type=F32)


def dot_nt(a, b):
    return lax.dot_general(a, b, (((1,), (1,)), ((), ())), preferred_element_type=F32)


def split(x):
    high = x.astype(BF16)
    return high, (x - high.astype(F32)).astype(BF16)


def left(constants, y):
    high, low = split(y)
    return dot(constants, jnp.concatenate([high, low, high, low], axis=0))


def right(x, high_constants, low_constants):
    high, low = split(x)
    return dot(high, high_constants) + dot(low, high_constants) + dot(high, low_constants)


def iota(shape, dim):
    return lax.broadcasted_iota(jnp.int32, shape, dim)


def kernel(
    total_count,
    g_hbm,
    m_hbm,
    idx_hbm,
    fwd_pair_hbm,
    inv_right_hbm,
    entry_hbm,
    inv_left_hbm,
    nm_ref,
    up_ref,
    idx_ref,
    fwd_pair,
    inv_right,
    entry,
    inv_left,
    g_ref,
    m_ref,
    y_ref,
    s_ref,
    ob_ref,
    oa_ref,
    turned_ref,
    il_ref,
    msg_ref,
    recv_ref,
    land_ref,
    ex_ref,
    ey_ref,
    ez_ref,
    const_sem,
    in_sem,
    msg_send,
    msg_recv,
    land_send,
    land_recv,
    e_send,
    e_recv,
):
    me = lax.axis_index("dp")
    tensor = lax.axis_index("tensor")
    z, y = me // RING, lax.rem(me, RING)
    replicas = RING * RING
    chunks = ob_ref.shape[0]
    groups = chunks // GROUP
    wide = GROUP * CHUNK

    def group_columns(i):
        return pl.ds(pl.multiple_of(i * wide, wide), wide)

    def load(i, which):
        hbm, ref = ((g_hbm, g_ref), (m_hbm, m_ref))[which]
        return pltpu.make_async_copy(
            hbm.at[0, :, group_columns(i)], ref.at[:, group_columns(i)], in_sem.at[which, i]
        )

    barrier = pltpu.get_barrier_semaphore()

    def greet_dp(k, carry):
        pl.semaphore_signal(barrier, inc=1, device_id={"dp": lax.rem(me + k, replicas)}, device_id_type=MESH)
        return carry

    def greet_tensor(k, carry):
        pl.semaphore_signal(barrier, inc=1, device_id={"tensor": lax.rem(tensor + k, RING)}, device_id_type=MESH)
        return carry

    lax.fori_loop(1, replicas, greet_dp, 0)
    lax.fori_loop(1, RING, greet_tensor, 0)

    small = [
        pltpu.make_async_copy(hbm, ref, const_sem.at[i])
        for i, (hbm, ref) in enumerate(
            [
                (idx_hbm, idx_ref),
                (entry_hbm, entry),
                (fwd_pair_hbm, fwd_pair),
                (inv_right_hbm, inv_right),
                (inv_left_hbm, inv_left),
            ]
        )
    ]
    for copy in small[:3]:
        copy.start()
    for i in range(groups):
        load(i, 0).start()
        load(i, 1).start()
    for copy in small[3:]:
        copy.start()

    small[0].wait()
    turned_ref[...] = jnp.transpose(idx_ref[...])
    il_ref[...] = jnp.concatenate(
        [turned_ref[pl.ds(k, chunks, stride=4), :] for k in range(4)], axis=1
    )
    lane_span = iota((1, 128), 1) // TOPK

    def mark(chunk, carry):
        ids = il_ref[pl.ds(chunk, 1), :]
        row_hit = iota((BLOCK, 128), 0) == ids // BLOCK
        col_hit = iota((CHUNK, 128), 0) == lax.rem(ids, BLOCK) + BLOCK * lane_span
        ob_ref[chunk] = jnp.where(col_hit, 1.0, 0.0).astype(BF16)
        oa_ref[chunk] = jnp.where(row_hit, 1.0, 0.0).astype(BF16)
        msg_ref[chunk, 1:2, :] = ids.astype(F32)
        return carry

    lax.fori_loop(0, chunks, mark, 0, unroll=2)

    def renewed(c):
        columns = pl.ds(pl.multiple_of(c * CHUNK, CHUNK), CHUNK)
        return DECAY * m_ref[:, columns].astype(F32) + g_ref[:, columns].astype(F32)

    small[1].wait()
    small[2].wait()

    def rows_first(i):
        load(i, 0).wait()
        load(i, 1).wait()
        for c in range(i * GROUP, (i + 1) * GROUP):
            columns = slice(c * CHUNK, (c + 1) * CHUNK)
            both = dot(entry[...], jnp.concatenate([m_ref[:, columns], g_ref[:, columns]], axis=0))
            high, low = split(both[:BLOCK] + both[BLOCK:])
            for k in range(2):
                rows = slice((2 * c + k) * BLOCK, (2 * c + k + 1) * BLOCK)
                y_ref[rows, :128] = high[:, k * 128 : (k + 1) * 128]
                y_ref[rows, 128:] = low[:, k * 128 : (k + 1) * 128]

    def columns_next(i):
        rows = slice(i * GROUP * 2 * BLOCK, (i + 1) * GROUP * 2 * BLOCK)
        both = dot(y_ref[rows, :], fwd_pair[...])
        s_ref[rows, :] = both[:, :128] + both[:, 128:]

    def spectrum_of(c):
        start = c * 2 * BLOCK
        return jnp.concatenate([s_ref[pl.ds(start, BLOCK), :], s_ref[pl.ds(start + BLOCK, BLOCK), :]], axis=1)

    def pick(i):
        for c in range(i * GROUP, (i + 1) * GROUP):
            by_column = dot(spectrum_of(c).astype(BF16), ob_ref[c])
            msg_ref[c, 0:1, :] = jnp.sum(by_column * oa_ref[c].astype(F32), axis=0, keepdims=True)

    for i in range(groups + 2):
        if i >= 2:
            pick(i - 2)
        if 1 <= i <= groups:
            columns_next(i - 1)
        if i < groups:
            rows_first(i)
    small[3].wait()
    small[4].wait()

    pl.semaphore_wait(barrier, replicas - 1 + RING - 1)

    def send_values(k, carry):
        peer = lax.rem(me + k, replicas)
        pltpu.make_async_remote_copy(
            src_ref=msg_ref.at[peer // 2],
            dst_ref=recv_ref.at[me],
            send_sem=msg_send,
            recv_sem=msg_recv,
            device_id={"dp": peer},
            device_id_type=MESH,
        ).start()
        return carry

    lax.fori_loop(1, replicas, send_values, 0)

    def remove(i, carry):
        rows = []
        for c in range(GROUP):
            chunk = i * GROUP + c
            marker = dot_nt(oa_ref[chunk], ob_ref[chunk])
            rows.append(split(left(inv_left[...], spectrum_of(chunk) * marker)))
        high = jnp.concatenate([r[0] for r in rows], axis=0)
        low = jnp.concatenate([r[1] for r in rows], axis=0)
        restored = dot(high, inv_right[0]) + dot(low, inv_right[0]) + dot(high, inv_right[1])
        for c in range(GROUP):
            chunk = i * GROUP + c
            columns = pl.ds(pl.multiple_of(chunk * CHUNK, CHUNK), CHUNK)
            nm_ref[:, columns] = (renewed(chunk) - restored[c * BLOCK : (c + 1) * BLOCK]).astype(BF16)
        return carry

    lax.fori_loop(0, groups, remove, 0)

    others = recv_ref.at[pl.ds(0, replicas - 1)]
    pltpu.make_async_copy(others, others, msg_recv).wait()
    recv_ref[me] = msg_ref[me // 2]

    odd = lax.rem(me, 2)
    lane = iota((replicas // 2, 128), 1)

    def mine(array):
        array = jnp.where(odd == 0, array, pltpu.roll(array, 64, 1))
        return jnp.where(lane < 64, array[: replicas // 2], pltpu.roll(array[replicas // 2 :], 64, 1))

    got_values = mine(recv_ref[:, 0, :])
    got_ids = mine(recv_ref[:, 1, :]).astype(jnp.int32)
    got_rows = got_ids // BLOCK
    got_cols = lax.rem(got_ids, BLOCK) + BLOCK * lax.rem(lane // TOPK, 2)
    combined = jnp.zeros((BLOCK, 128), F32)
    for r in range(0, replicas // 2, 2):
        rows, cols = [], []
        for k in (r, r + 1):
            rows.append(
                jnp.where(iota((BLOCK, 128), 0) == got_rows[k : k + 1], got_values[k : k + 1], 0.0).astype(BF16)
            )
            cols.append(jnp.where(iota((128, 128), 0) == got_cols[k : k + 1], 1.0, 0.0).astype(BF16))
        combined += dot_nt(jnp.concatenate(rows, axis=1), jnp.concatenate(cols, axis=1))
    decoded = left(inv_left[...], right(combined, inv_right[0, :128, :128], inv_right[1, :128, :128]))
    rounded = decoded.astype(BF16)
    half_rows = BLOCK // 2
    land_ref[0, me] = rounded[:half_rows]
    land_ref[1, me] = rounded[half_rows:]

    energy_refs = (ex_ref, ey_ref, ez_ref)
    energy_places = (tensor, y, z)

    def energy_target(stage, place):
        if stage == 0:
            return {"tensor": place}
        return {"dp": z * RING + place if stage == 1 else place * RING + y}

    def send_energy(stage, row):
        ref, place = energy_refs[stage], energy_places[stage]
        ref[place] = row

        def send(k, carry):
            peer = lax.rem(place + k, RING)
            pltpu.make_async_remote_copy(
                src_ref=ref.at[place],
                dst_ref=ref.at[place],
                send_sem=e_send.at[stage],
                recv_sem=e_recv.at[stage],
                device_id=energy_target(stage, peer),
                device_id_type=MESH,
            ).start()
            return carry

        lax.fori_loop(1, RING, send, 0)

    def take_energy(stage):
        ref = energy_refs[stage]
        rest = ref.at[pl.ds(0, RING - 1)]
        pltpu.make_async_copy(rest, rest, e_recv.at[stage]).wait()
        pltpu.make_async_copy(rest, rest, e_send.at[stage]).wait()
        row = ref[0]
        for k in range(1, RING):
            row = row + ref[k]
        return row

    send_energy(0, jnp.sum(decoded * decoded, axis=0, keepdims=True))

    along = ((y, z), (z, y))

    def place_of(h, a, b):
        a, b = lax.rem(a + 2 * RING, RING), lax.rem(b + 2 * RING, RING)
        return b * RING + a if h == 0 else a * RING + b

    def send_item(h, item, target):
        pltpu.make_async_remote_copy(
            src_ref=land_ref.at[h, item],
            dst_ref=land_ref.at[h, item],
            send_sem=land_send.at[h],
            recv_sem=land_recv.at[h, item],
            device_id={"dp": target},
            device_id_type=MESH,
        ).start()

    def wait_item(h, item):
        ref = land_ref.at[h, item]
        pltpu.make_async_copy(ref, ref, land_recv.at[h, item]).wait()

    def nearest(i):
        return ((i + 1) // 2) * (2 * lax.rem(i, 2) - 1)

    def first_sends(i, carry):
        for h in range(2):
            a, b = along[h]
            send_item(h, me, place_of(h, a + nearest(RING - i), b))
        return carry

    lax.fori_loop(1, RING, first_sends, 0)

    def spread(h, item):
        a, b = along[h]
        for step in (2, -2, 1, -1):
            send_item(h, item, place_of(h, a, b + step))

    for h in range(2):
        spread(h, me)

    def second_sends(i, carry):
        for h in range(2):
            a, b = along[h]
            item = place_of(h, a + nearest(i), b)
            wait_item(h, item)
            spread(h, item)
        return carry

    lax.fori_loop(1, 4, second_sends, 0)
    send_energy(1, take_energy(0))
    lax.fori_loop(4, RING, second_sends, 0)

    def third_sends(i, carry):
        for h in range(2):
            a, b = along[h]
            other = a + jnp.where(i == 0, 0, nearest(i))
            other = lax.rem(other + RING, RING)
            for step in (2, -2):
                item = place_of(h, other, b - step)
                wait_item(h, item)
                send_item(h, item, place_of(h, a, b + step // 2))
            sign = 1 - 2 * lax.rem(other, 2)
            send_item(h, place_of(h, other, b - 2 * sign), place_of(h, a, b + 2 * sign))
        return carry

    lax.fori_loop(0, 4, third_sends, 0)
    send_energy(2, take_energy(1))
    lax.fori_loop(4, RING, third_sends, 0)

    energy = jnp.sum(take_energy(2), axis=1, keepdims=True)
    scale = 1.0 / jnp.sqrt(energy / total_count + EPSILON)

    def last_waits(i, carry):
        for h in range(2):
            b = along[h][1]
            for step in (1, -1, 3, -3, 4):
                wait_item(h, place_of(h, i, b + step))
        return carry

    lax.fori_loop(0, RING, last_waits, 0)

    per_group = wide // 128

    def finish(i, carry):
        for k in range(per_group):
            item = i * per_group + k
            columns = pl.ds(pl.multiple_of(item * 128, 128), 128)
            for h in range(2):
                up_ref[h * half_rows : (h + 1) * half_rows, columns] = (
                    land_ref[h, item].astype(F32) * scale
                ).astype(BF16)
        return carry

    lax.fori_loop(0, groups, finish, 0)

    pltpu.make_async_copy(others, others, msg_send).wait()
    for h in range(2):
        rest = land_ref.at[h, pl.ds(0, replicas - 1)]
        pltpu.make_async_copy(rest, rest, land_send.at[h]).wait()


def local(total_count, gradient, momentum, indices):
    _, height, columns = gradient.shape
    chunks = columns // CHUNK
    groups = chunks // GROUP
    replicas = RING * RING
    cosines = basis()
    anywhere = pl.BlockSpec(memory_space=pl.ANY)
    dma = pltpu.SemaphoreType.DMA
    nm, up = pl.pallas_call(
        functools.partial(kernel, total_count),
        out_shape=(
            pltpu.VMEM((height, columns), BF16),
            pltpu.VMEM((height, columns), BF16),
        ),
        in_specs=[anywhere] * 7,
        out_specs=(pl.BlockSpec(memory_space=pltpu.VMEM),) * 2,
        scratch_shapes=[
            pltpu.VMEM((TOPK, columns // BLOCK), jnp.int32),
            pltpu.VMEM((256, 256), BF16),
            pltpu.VMEM((2, 256, 256), BF16),
            pltpu.VMEM((128, 128), BF16),
            pltpu.VMEM((BLOCK, 256), BF16),
            pltpu.VMEM((height, columns), BF16),
            pltpu.VMEM((height, columns), BF16),
            pltpu.VMEM((chunks * 2 * BLOCK, 256), BF16),
            pltpu.VMEM((chunks * 2 * BLOCK, 128), F32),
            pltpu.VMEM((chunks, CHUNK, 128), BF16),
            pltpu.VMEM((chunks, BLOCK, 128), BF16),
            pltpu.VMEM((chunks * 4, TOPK), jnp.int32),
            pltpu.VMEM((chunks, 128), jnp.int32),
            pltpu.VMEM((chunks, 2, 128), F32),
            pltpu.VMEM((replicas, 2, 128), F32),
            pltpu.VMEM((2, replicas, BLOCK // 2, 128), BF16),
            pltpu.VMEM((RING, 1, 128), F32),
            pltpu.VMEM((RING, 1, 128), F32),
            pltpu.VMEM((RING, 1, 128), F32),
            dma((5,)),
            dma((2, groups)),
            dma,
            dma,
            dma((2,)),
            dma((2, replicas)),
            dma((3,)),
            dma((3,)),
        ],
        compiler_params=pltpu.CompilerParams(collective_id=0, has_side_effects=True, vmem_limit_bytes=64880640),
        name="demo_step",
    )(
        gradient,
        momentum,
        jnp.transpose(indices.reshape(columns // BLOCK, TOPK)),
        pair_constants(cosines.T),
        right_constants(cosines),
        entry_constants(cosines),
        left_constants(cosines.T),
    )
    return nm[None], up


def solution(mesh):
    def whole(gradient, momentum, indices):
        rows, columns = gradient.shape[1:]
        return jax.shard_map(
            functools.partial(local, float(rows * columns)),
            mesh=mesh,
            in_specs=(P("dp", "tensor", None), P("dp", "tensor", None), P("dp", "tensor", None, None)),
            out_specs=(P("dp", "tensor", None), P("tensor", None)),
            check_vma=False,
        )(gradient, momentum, indices)

    return whole
```

```python
import functools

import jax
import jax.numpy as jnp
import numpy as np
from jax import lax
from jax.experimental import pallas as pl
from jax.experimental.pallas import tpu as pltpu
from jax.sharding import PartitionSpec as P

MESH = pl.DeviceIdType.MESH
BLOCK = 64
TOPK = 32
CHUNK = 256
RING = 8
OWN = 4
GROUP = 8
EPSILON = 1e-06
DECAY = 0.999
F32 = jnp.float32
BF16 = jnp.bfloat16


def basis():
    frequency = np.arange(BLOCK, dtype=np.float64)[:, None]
    position = np.arange(BLOCK, dtype=np.float64)[None, :]
    waves = np.cos(np.pi * (2.0 * position + 1.0) * frequency / (2.0 * BLOCK))
    return waves * np.where(frequency == 0.0, np.sqrt(1.0 / BLOCK), np.sqrt(2.0 / BLOCK))


def halves(array):
    array = array.astype(np.float32)
    high = array.astype(BF16)
    low = (array - high.astype(np.float32)).astype(BF16)
    return high, low


def pair_constants(matrix):
    pair = np.concatenate([np.kron(np.eye(2), half.astype(np.float32)).astype(BF16) for half in halves(matrix)], axis=1)
    return np.concatenate([pair, pair], axis=0)


def entry_constants(matrix):
    return np.concatenate(
        [np.concatenate(pair, axis=1) for pair in zip(halves(DECAY * matrix), halves(matrix))], axis=0
    )


def left_constants(matrix):
    high, low = halves(matrix)
    return np.concatenate([high, high, low, low], axis=1)


def dot(a, b):
    return jnp.dot(a, b, preferred_element_type=F32)


def dot_nt(a, b):
    return lax.dot_general(a, b, (((1,), (1,)), ((), ())), preferred_element_type=F32)


def split(x):
    high = x.astype(BF16)
    return high, (x - high.astype(F32)).astype(BF16)


def left(constants, y):
    high, low = split(y)
    return dot(constants, jnp.concatenate([high, low, high, low], axis=0))


def iota(shape, dim):
    return lax.broadcasted_iota(jnp.int32, shape, dim)


def kernel(
    total_count,
    g_hbm,
    m_hbm,
    idx_hbm,
    fwd_pair_hbm,
    inv_pair_hbm,
    entry_hbm,
    inv_left_hbm,
    nm_ref,
    up_ref,
    idx_ref,
    fwd_pair,
    inv_pair,
    entry,
    inv_left,
    g_ref,
    m_ref,
    y_ref,
    s_ref,
    ob_ref,
    oa_ref,
    turned_ref,
    il_ref,
    sent_ids,
    msg_ref,
    recv_ids,
    recv_values,
    flat_ids,
    flat_values,
    part_ref,
    land_ref,
    et_ref,
    ed_ref,
    const_sem,
    in_sem,
    msg_send,
    msg_recv,
    land_send,
    land_recv,
    e_send,
    e_recv,
):
    me = lax.axis_index("dp")
    tensor = lax.axis_index("tensor")
    z, y = me // RING, lax.rem(me, RING)
    replicas = RING * RING
    chunks = ob_ref.shape[0]
    groups = chunks // GROUP
    wide = GROUP * CHUNK

    def group_columns(i):
        return pl.ds(pl.multiple_of(i * wide, wide), wide)

    def load(i, which):
        hbm, ref = ((g_hbm, g_ref), (m_hbm, m_ref))[which]
        return pltpu.make_async_copy(
            hbm.at[0, :, group_columns(i)], ref.at[:, group_columns(i)], in_sem.at[which, i]
        )

    small = [
        pltpu.make_async_copy(hbm, ref, const_sem.at[i])
        for i, (hbm, ref) in enumerate(
            [
                (idx_hbm, idx_ref),
                (entry_hbm, entry),
                (fwd_pair_hbm, fwd_pair),
                (inv_pair_hbm, inv_pair),
                (inv_left_hbm, inv_left),
            ]
        )
    ]
    for copy in small[:3]:
        copy.start()
    for i in range(groups):
        load(i, 0).start()
        load(i, 1).start()
    for copy in small[3:]:
        copy.start()

    barrier = pltpu.get_barrier_semaphore()

    def nearest(i):
        return ((i + 1) // 2) * (2 * lax.rem(i, 2) - 1)

    def far_first(i, visit, own):
        peer_z = lax.rem(z + nearest(RING - 1 - i) + RING, RING)
        for step in (4, 3, -3, 2, -2, 1, -1):
            visit(peer_z * RING + lax.rem(y + step + RING, RING))
        if not own:
            visit(peer_z * RING + y)

    def every_peer(visit):
        def row(i, carry):
            far_first(i, visit, False)
            return carry

        lax.fori_loop(0, RING - 1, row, 0)
        far_first(RING - 1, visit, True)

    def greet(peer):
        pl.semaphore_signal(barrier, inc=1, device_id={"dp": peer}, device_id_type=MESH)

    def greet_tensor(k, carry):
        pl.semaphore_signal(barrier, inc=1, device_id={"tensor": lax.rem(tensor + k, RING)}, device_id_type=MESH)
        return carry

    every_peer(greet)
    lax.fori_loop(1, RING, greet_tensor, 0)

    small[0].wait()
    turned_ref[...] = jnp.transpose(idx_ref[...])
    il_ref[...] = jnp.concatenate(
        [turned_ref[pl.ds(k, chunks, stride=4), :] for k in range(4)], axis=1
    )
    lane_span = iota((1, 128), 1) // TOPK

    def mark(chunk):
        ids = il_ref[chunk : chunk + 1, :]
        row_hit = iota((BLOCK, 128), 0) == ids // BLOCK
        col_hit = iota((CHUNK, 128), 0) == lax.rem(ids, BLOCK) + BLOCK * lane_span
        ob_ref[chunk] = jnp.where(col_hit, 1.0, 0.0).astype(BF16)
        oa_ref[chunk] = jnp.where(row_hit, 1.0, 0.0).astype(BF16)
        sent_ids[chunk // 2, chunk % 2 : chunk % 2 + 1, :] = ids

    def renewed(c):
        columns = pl.ds(pl.multiple_of(c * CHUNK, CHUNK), CHUNK)
        return DECAY * m_ref[:, columns].astype(F32) + g_ref[:, columns].astype(F32)

    small[1].wait()
    small[2].wait()

    def rows_first(i):
        load(i, 0).wait()
        load(i, 1).wait()
        for c in range(i * GROUP, (i + 1) * GROUP):
            columns = slice(c * CHUNK, (c + 1) * CHUNK)
            both = dot(entry[...], jnp.concatenate([m_ref[:, columns], g_ref[:, columns]], axis=0))
            high, low = split(both[:BLOCK] + both[BLOCK:])
            for k in range(2):
                rows = slice((2 * c + k) * BLOCK, (2 * c + k + 1) * BLOCK)
                y_ref[rows, :128] = high[:, k * 128 : (k + 1) * 128]
                y_ref[rows, 128:] = low[:, k * 128 : (k + 1) * 128]

    def columns_next(i):
        rows = slice(i * GROUP * 2 * BLOCK, (i + 1) * GROUP * 2 * BLOCK)
        both = dot(y_ref[rows, :], fwd_pair[...])
        s_ref[rows, :] = both[:, :128] + both[:, 128:]

    def spectrum_of(c):
        start = c * 2 * BLOCK
        return jnp.concatenate([s_ref[pl.ds(start, BLOCK), :], s_ref[pl.ds(start + BLOCK, BLOCK), :]], axis=1)

    def pick(i):
        for c in range(i * GROUP, (i + 1) * GROUP):
            by_column = dot(spectrum_of(c).astype(BF16), ob_ref[c])
            row = jnp.sum(by_column * oa_ref[c].astype(F32), axis=0, keepdims=True)
            if c % 2:
                msg_ref[c // 2] = jnp.concatenate([before, row], axis=0).astype(BF16)
            before = row

    for i in range(groups + 2):
        if i >= 2:
            pick(i - 2)
        if 1 <= i <= groups:
            columns_next(i - 1)
        if i < groups:
            rows_first(i)
            for c in range(i * GROUP, (i + 1) * GROUP):
                mark(c)

    pl.semaphore_wait(barrier, replicas - 1 + RING - 1)

    def owned(place):
        return lax.rem(place // RING, OWN) * OWN + lax.rem(place, OWN)

    def send_messages(peer):
        for i, (source, target) in enumerate(((sent_ids, recv_ids), (msg_ref, recv_values))):
            pltpu.make_async_remote_copy(
                src_ref=source.at[owned(peer)],
                dst_ref=target.at[me],
                send_sem=msg_send.at[i],
                recv_sem=msg_recv.at[i, z],
                device_id={"dp": peer},
                device_id_type=MESH,
            ).start()

    every_peer(send_messages)

    def paired(pieces):
        rows = []
        for piece in pieces:
            high, low = split(piece)
            for k in range(0, piece.shape[1], 128):
                rows.append(jnp.concatenate([high[:, k : k + 128], low[:, k : k + 128]], axis=1))
        both = dot(jnp.concatenate(rows, axis=0), inv_pair[...])
        both = both[:, :128] + both[:, 128:]
        return [both[k * BLOCK : (k + 1) * BLOCK] for k in range(len(rows))]

    small[3].wait()
    small[4].wait()
    mine = owned(me)
    recv_ids[me] = sent_ids[mine]
    recv_values[me] = msg_ref[mine]

    frequency = iota((BLOCK, 128), 0)
    lane_group = iota((RING, 128), 1) // TOPK
    own_group = lax.rem(iota((RING, 128), 0), 4) == lane_group

    def turns(rows):
        return [rows] + [pltpu.roll(rows, TOPK * k, 1) for k in range(1, 4)]

    def gathered(turned, k):
        out = turned[(-k) % 4]
        for g in range(1, 4):
            out = jnp.where(lane_group == g, turned[(g - k) % 4], out)
        out = jnp.where(own_group, out, jnp.zeros_like(out))
        out = out + pltpu.roll(out, 1, 0)
        return out + pltpu.roll(out, 2, 0)

    def combine(row, count):
        for i, ref in enumerate((recv_ids, recv_values)):
            arrived = ref.at[pl.ds(0, count)]
            pltpu.make_async_copy(arrived, arrived, msg_recv.at[i, row]).wait()
        flat_ids[...] = recv_ids[pl.ds(row * RING, RING)].reshape(2 * RING, 128)
        flat_values[...] = recv_values[pl.ds(row * RING, RING)].astype(F32).reshape(2 * RING, 128)
        for u in range(2):
            all_ids = turns(flat_ids[pl.ds(u, RING, stride=2), :])
            all_values = turns(flat_values[pl.ds(u, RING, stride=2), :])
            for k in range(4):
                ids, values = gathered(all_ids, k), gathered(all_values, k)
                ids_a, ids_b = ids // BLOCK, lax.rem(ids, BLOCK)
                rows, cols = [], []
                for j in (3, 7):
                    rows.append(jnp.where(frequency == ids_a[j : j + 1], values[j : j + 1], 0.0).astype(BF16))
                    cols.append(jnp.where(frequency == ids_b[j : j + 1], 1.0, 0.0).astype(BF16))
                part_ref[row, 4 * u + k] = dot_nt(jnp.concatenate(rows, axis=1), jnp.concatenate(cols, axis=1))

    combine(z, RING - 1)

    def combine_row(i, carry):
        combine(lax.rem(z + nearest(i) + RING, RING), RING)
        return carry

    lax.fori_loop(1, RING, combine_row, 0)

    def summed(k):
        total = part_ref[0, k]
        for row in range(1, RING):
            total = total + part_ref[row, k]
        return total

    combined = [jnp.concatenate([summed(k), summed(k + 1)], axis=1) for k in range(0, 8, 2)]
    energy = sum(jnp.sum(pair * pair, axis=0, keepdims=True) for pair in combined)

    def send_energy(ref, place, stage, targets):
        for target in targets:
            pltpu.make_async_remote_copy(
                src_ref=ref.at[place],
                dst_ref=ref.at[place],
                send_sem=e_send.at[stage],
                recv_sem=e_recv.at[stage],
                device_id=target,
                device_id_type=MESH,
            ).start()

    et_ref[tensor] = energy
    send_energy(et_ref, tensor, 0, [{"tensor": lax.rem(tensor + k, RING)} for k in (4, 5, 3, 2, 6, 7, 1)])

    halfway = paired(combined)
    quarter_rows = BLOCK // 4
    for k in range(2):
        decoded = left(inv_left[...], jnp.concatenate(halfway[2 * k : 2 * k + 2], axis=1))
        rounded = decoded.astype(BF16)
        for h in range(2):
            for part in range(2):
                start = (2 * h + part) * quarter_rows
                land_ref[h, mine, part, :, k * CHUNK : (k + 1) * CHUNK] = rounded[start : start + quarter_rows]

    along = ((y, z), (z, y))

    def place_of(h, a, b):
        a, b = lax.rem(a + RING, RING), lax.rem(b + RING, RING)
        return b * RING + a if h == 0 else a * RING + b

    def item_of(h, a, b):
        return owned(place_of(h, a, b))

    def send_item(h, ref, sem, target):
        pltpu.make_async_remote_copy(
            src_ref=ref,
            dst_ref=ref,
            send_sem=land_send.at[h],
            recv_sem=sem,
            device_id={"dp": target},
            device_id_type=MESH,
        ).start()

    def spread(h, item, places):
        for step, place in zip((1, -1), places[:2]):
            send_item(h, land_ref.at[h, item], land_recv.at[h, item, 0], place)
        for part, place in enumerate(places[2:]):
            send_item(h, land_ref.at[h, item, part], land_recv.at[h, item, part], place)

    def spread_first(h):
        a, b = along[h]
        spread(h, mine, [place_of(h, a + step, b) for step in (1, -1, 2, -2)])

    def spread_second(h, item):
        a, b = along[h]
        spread(h, item, [place_of(h, a, b + step) for step in (1, -1, 2, -2)])

    def wait_whole(h, item):
        ref = land_ref.at[h, item]
        pltpu.make_async_copy(ref, ref, land_recv.at[h, item, 0]).wait()

    def wait_parts(h, item):
        for part in range(2):
            ref = land_ref.at[h, item, part]
            pltpu.make_async_copy(ref, ref, land_recv.at[h, item, part]).wait()

    def take_energy(ref, stage, count):
        rest = ref.at[pl.ds(0, count - 1)]
        pltpu.make_async_copy(rest, rest, e_recv.at[stage]).wait()
        pltpu.make_async_copy(rest, rest, e_send.at[stage]).wait()
        row = ref[0]
        for k in range(1, count):
            row = row + ref[k]
        return row

    for h in range(2):
        spread_first(h)
    for h in range(2):
        spread_second(h, mine)
    for step in (1, -1):
        for h in range(2):
            a, b = along[h]
            item = item_of(h, a + step, b)
            wait_whole(h, item)
            spread_second(h, item)
    ed_ref[mine] = take_energy(et_ref, 0, RING)
    near = [(i, j) for i in (-1, 0, 1, 2) for j in (-1, 0, 1, 2) if (i, j) != (0, 0)]
    send_energy(ed_ref, mine, 1, [{"dp": place_of(0, y + i, z + j)} for i, j in near])
    for h in range(2):
        a, b = along[h]
        item = item_of(h, a + 2, b)
        wait_parts(h, item)
        spread_second(h, item)

    def remove(i, carry):
        rows = []
        for c in range(GROUP):
            chunk = i * GROUP + c
            marker = dot_nt(oa_ref[chunk], ob_ref[chunk])
            rows.append(left(inv_left[...], spectrum_of(chunk) * marker))
        restored = paired(rows)
        for c in range(GROUP):
            chunk = i * GROUP + c
            columns = pl.ds(pl.multiple_of(chunk * CHUNK, CHUNK), CHUNK)
            taken = jnp.concatenate(restored[2 * c : 2 * c + 2], axis=1)
            nm_ref[:, columns] = (renewed(chunk) - taken).astype(BF16)
        return carry

    lax.fori_loop(0, groups, remove, 0)

    energy = jnp.sum(take_energy(ed_ref, 1, OWN * OWN), axis=1, keepdims=True)
    scale = 1.0 / jnp.sqrt(energy / total_count + EPSILON)

    def finish(h, item):
        columns = pl.ds(pl.multiple_of(item * 2 * CHUNK, 2 * CHUNK), 2 * CHUNK)
        for part in range(2):
            start = (2 * h + part) * quarter_rows
            up_ref[start : start + quarter_rows, columns] = (
                land_ref[h, item, part].astype(F32) * scale
            ).astype(BF16)

    steps = (0, 1, -1, 2)
    for other in steps:
        for step in steps:
            for h in range(2):
                a, b = along[h]
                item = item_of(h, a + step, b + other)
                if other in (1, -1):
                    wait_whole(h, item)
                elif other == 2:
                    wait_parts(h, item)
                finish(h, item)

    for i, ref in enumerate((recv_ids, recv_values)):
        others = ref.at[pl.ds(0, replicas - 1)]
        pltpu.make_async_copy(others, others, msg_send.at[i]).wait()
    for h in range(2):
        rest = land_ref.at[h, pl.ds(0, OWN * OWN - 1)]
        pltpu.make_async_copy(rest, rest, land_send.at[h]).wait()


def deliver(nm_ref, up_ref, nm_hbm, up_hbm, sem):
    copies = [
        pltpu.make_async_copy(nm_ref, nm_hbm.at[0], sem.at[0]),
        pltpu.make_async_copy(up_ref, up_hbm, sem.at[1]),
    ]
    for copy in copies:
        copy.start()
    for copy in copies:
        copy.wait()


def local(total_count, gradient, momentum, indices):
    _, height, columns = gradient.shape
    chunks = columns // CHUNK
    groups = chunks // GROUP
    replicas = RING * RING
    cosines = basis()
    anywhere = pl.BlockSpec(memory_space=pl.ANY)
    dma = pltpu.SemaphoreType.DMA
    nm, up = pl.pallas_call(
        functools.partial(kernel, total_count),
        out_shape=(
            pltpu.VMEM((height, columns), BF16),
            pltpu.VMEM((height, columns), BF16),
        ),
        in_specs=[anywhere] * 7,
        out_specs=(pl.BlockSpec(memory_space=pltpu.VMEM),) * 2,
        scratch_shapes=[
            pltpu.VMEM((TOPK, columns // BLOCK), jnp.int32),
            pltpu.VMEM((256, 256), BF16),
            pltpu.VMEM((256, 256), BF16),
            pltpu.VMEM((128, 128), BF16),
            pltpu.VMEM((BLOCK, 256), BF16),
            pltpu.VMEM((height, columns), BF16),
            pltpu.VMEM((height, columns), BF16),
            pltpu.VMEM((chunks * 2 * BLOCK, 256), BF16),
            pltpu.VMEM((chunks * 2 * BLOCK, 128), F32),
            pltpu.VMEM((chunks, CHUNK, 128), BF16),
            pltpu.VMEM((chunks, BLOCK, 128), BF16),
            pltpu.VMEM((chunks * 4, TOPK), jnp.int32),
            pltpu.VMEM((chunks, 128), jnp.int32),
            pltpu.VMEM((OWN * OWN, 2, 128), jnp.int32),
            pltpu.VMEM((OWN * OWN, 2, 128), BF16),
            pltpu.VMEM((replicas, 2, 128), jnp.int32),
            pltpu.VMEM((replicas, 2, 128), BF16),
            pltpu.VMEM((2 * RING, 128), jnp.int32),
            pltpu.VMEM((2 * RING, 128), F32),
            pltpu.VMEM((RING, 8, BLOCK, BLOCK), F32),
            pltpu.VMEM((2, OWN * OWN, 2, BLOCK // 4, 2 * CHUNK), BF16),
            pltpu.VMEM((RING, 1, 128), F32),
            pltpu.VMEM((OWN * OWN, 1, 128), F32),
            dma((5,)),
            dma((2, groups)),
            dma((2,)),
            dma((2, RING)),
            dma((2,)),
            dma((2, OWN * OWN, 2)),
            dma((2,)),
            dma((2,)),
        ],
        compiler_params=pltpu.CompilerParams(collective_id=0, has_side_effects=True, vmem_limit_bytes=64880640),
        name="demo_step",
    )(
        gradient,
        momentum,
        jnp.transpose(indices.reshape(columns // BLOCK, TOPK)),
        pair_constants(cosines.T),
        pair_constants(cosines),
        entry_constants(cosines),
        left_constants(cosines.T),
    )
    return pl.pallas_call(
        deliver,
        out_shape=(
            jax.ShapeDtypeStruct((1, height, columns), BF16),
            jax.ShapeDtypeStruct((height, columns), BF16),
        ),
        in_specs=[pl.BlockSpec(memory_space=pltpu.VMEM)] * 2,
        out_specs=(anywhere, anywhere),
        scratch_shapes=[dma((2,))],
        compiler_params=pltpu.CompilerParams(vmem_limit_bytes=2**20),
        name="deliver",
    )(nm, up)


def solution(mesh):
    def whole(gradient, momentum, indices):
        rows, columns = gradient.shape[1:]
        return jax.shard_map(
            functools.partial(local, float(rows * columns)),
            mesh=mesh,
            in_specs=(P("dp", "tensor", None), P("dp", "tensor", None), P("dp", "tensor", None, None)),
            out_specs=(P("dp", "tensor", None), P("tensor", None)),
            check_vma=False,
        )(gradient, momentum, indices)

    return whole
```

```python
import functools

import jax
import jax.numpy as jnp
import numpy as np
from jax import lax
from jax.experimental import pallas as pl
from jax.experimental.pallas import tpu as pltpu
from jax.sharding import PartitionSpec as P

MESH = pl.DeviceIdType.MESH
BLOCK = 64
TOPK = 32
CHUNK = 256
RING = 8
OWN = 4
GROUP = 16
EPSILON = 1e-06
DECAY = 0.999
F32 = jnp.float32
BF16 = jnp.bfloat16


def basis():
    frequency = np.arange(BLOCK, dtype=np.float64)[:, None]
    position = np.arange(BLOCK, dtype=np.float64)[None, :]
    waves = np.cos(np.pi * (2.0 * position + 1.0) * frequency / (2.0 * BLOCK))
    return waves * np.where(frequency == 0.0, np.sqrt(1.0 / BLOCK), np.sqrt(2.0 / BLOCK))


def halves(array):
    array = array.astype(np.float32)
    high = array.astype(BF16)
    low = (array - high.astype(np.float32)).astype(BF16)
    return high, low


def pair_constants(matrix):
    pair = np.concatenate([np.kron(np.eye(2), half.astype(np.float32)).astype(BF16) for half in halves(matrix)], axis=1)
    return np.concatenate([pair, pair], axis=0)


def entry_constants(matrix):
    return np.concatenate(
        [np.concatenate(pair, axis=1) for pair in zip(halves(DECAY * matrix), halves(matrix))], axis=0
    )


def left_constants(matrix):
    high, low = halves(matrix)
    return np.concatenate([high, high, low, low], axis=1)


def dot(a, b):
    return jnp.dot(a, b, preferred_element_type=F32)


def dot_nt(a, b):
    return lax.dot_general(a, b, (((1,), (1,)), ((), ())), preferred_element_type=F32)


def split(x):
    high = x.astype(BF16)
    return high, (x - high.astype(F32)).astype(BF16)


def left(constants, y):
    high, low = split(y)
    return dot(constants, jnp.concatenate([high, low, high, low], axis=0))


def iota(shape, dim):
    return lax.broadcasted_iota(jnp.int32, shape, dim)


def kernel(
    total_count,
    g_hbm,
    m_hbm,
    idx_hbm,
    fwd_pair_hbm,
    inv_pair_hbm,
    entry_hbm,
    inv_left_hbm,
    nm_ref,
    up_ref,
    idx_ref,
    fwd_pair,
    inv_pair,
    entry,
    inv_left,
    g_ref,
    m_ref,
    y_ref,
    s_ref,
    ob_ref,
    oa_ref,
    turned_ref,
    il_ref,
    sent_ids,
    msg_ref,
    recv_ids,
    recv_values,
    flat_ids,
    flat_values,
    part_ref,
    land_ref,
    et_ref,
    ed_ref,
    const_sem,
    in_sem,
    msg_send,
    msg_recv,
    land_send,
    land_recv,
    e_send,
    e_recv,
):
    me = lax.axis_index("dp")
    tensor = lax.axis_index("tensor")
    z, y = me // RING, lax.rem(me, RING)
    replicas = RING * RING
    chunks = ob_ref.shape[0]
    groups = chunks // GROUP
    wide = GROUP * CHUNK

    def group_columns(i):
        return pl.ds(pl.multiple_of(i * wide, wide), wide)

    def load(i, which):
        hbm, ref = ((g_hbm, g_ref), (m_hbm, m_ref))[which]
        return pltpu.make_async_copy(
            hbm.at[0, :, group_columns(i)], ref.at[:, group_columns(i)], in_sem.at[which, i]
        )

    small = [
        pltpu.make_async_copy(hbm, ref, const_sem.at[i])
        for i, (hbm, ref) in enumerate(
            [
                (idx_hbm, idx_ref),
                (entry_hbm, entry),
                (fwd_pair_hbm, fwd_pair),
                (inv_pair_hbm, inv_pair),
                (inv_left_hbm, inv_left),
            ]
        )
    ]
    for copy in small[:3]:
        copy.start()
    for i in range(groups):
        load(i, 0).start()
        load(i, 1).start()
    for copy in small[3:]:
        copy.start()

    barrier = pltpu.get_barrier_semaphore()

    def nearest(i):
        return ((i + 1) // 2) * (2 * lax.rem(i, 2) - 1)

    def far_first(i, visit, own):
        peer_z = lax.rem(z + nearest(RING - 1 - i) + RING, RING)
        for step in (4, 3, -3, 2, -2, 1, -1):
            visit(peer_z * RING + lax.rem(y + step + RING, RING))
        if not own:
            visit(peer_z * RING + y)

    def every_peer(visit):
        def row(i, carry):
            far_first(i, visit, False)
            return carry

        lax.fori_loop(0, RING - 1, row, 0)
        far_first(RING - 1, visit, True)

    def greet(peer):
        pl.semaphore_signal(barrier, inc=1, device_id={"dp": peer}, device_id_type=MESH)

    def greet_tensor(k, carry):
        pl.semaphore_signal(barrier, inc=1, device_id={"tensor": lax.rem(tensor + k, RING)}, device_id_type=MESH)
        return carry

    every_peer(greet)
    lax.fori_loop(1, RING, greet_tensor, 0)

    small[0].wait()
    turned_ref[...] = jnp.transpose(idx_ref[...])
    il_ref[...] = jnp.concatenate(
        [turned_ref[pl.ds(k, chunks, stride=4), :] for k in range(4)], axis=1
    )
    lane_span = iota((1, 128), 1) // TOPK

    def mark(chunk):
        ids = il_ref[chunk : chunk + 1, :]
        row_hit = iota((BLOCK, 128), 0) == ids // BLOCK
        col_hit = iota((CHUNK, 128), 0) == lax.rem(ids, BLOCK) + BLOCK * lane_span
        ob_ref[chunk] = jnp.where(col_hit, 1.0, 0.0).astype(BF16)
        oa_ref[chunk] = jnp.where(row_hit, 1.0, 0.0).astype(BF16)
        sent_ids[chunk // 2, chunk % 2 : chunk % 2 + 1, :] = ids

    def renewed(c):
        columns = pl.ds(pl.multiple_of(c * CHUNK, CHUNK), CHUNK)
        return DECAY * m_ref[:, columns].astype(F32) + g_ref[:, columns].astype(F32)

    small[1].wait()
    small[2].wait()

    def rows_first(i):
        load(i, 0).wait()
        load(i, 1).wait()
        for c in range(i * GROUP, (i + 1) * GROUP):
            columns = slice(c * CHUNK, (c + 1) * CHUNK)
            both = dot(entry[...], jnp.concatenate([m_ref[:, columns], g_ref[:, columns]], axis=0))
            high, low = split(both[:BLOCK] + both[BLOCK:])
            for k in range(2):
                rows = slice((2 * c + k) * BLOCK, (2 * c + k + 1) * BLOCK)
                y_ref[rows, :128] = high[:, k * 128 : (k + 1) * 128]
                y_ref[rows, 128:] = low[:, k * 128 : (k + 1) * 128]

    def columns_next(i):
        rows = slice(i * GROUP * 2 * BLOCK, (i + 1) * GROUP * 2 * BLOCK)
        both = dot(y_ref[rows, :], fwd_pair[...])
        s_ref[rows, :] = both[:, :128] + both[:, 128:]

    def spectrum_of(c):
        start = c * 2 * BLOCK
        return jnp.concatenate([s_ref[pl.ds(start, BLOCK), :], s_ref[pl.ds(start + BLOCK, BLOCK), :]], axis=1)

    def pick(i):
        for c in range(i * GROUP, (i + 1) * GROUP):
            by_column = dot(spectrum_of(c).astype(BF16), ob_ref[c])
            row = jnp.sum(by_column * oa_ref[c].astype(F32), axis=0, keepdims=True)
            if c % 2:
                msg_ref[c // 2] = jnp.concatenate([before, row], axis=0).astype(BF16)
            before = row

    for i in range(groups + 2):
        if i >= 2:
            pick(i - 2)
        if 1 <= i <= groups:
            columns_next(i - 1)
        if i < groups:
            rows_first(i)
            for c in range(i * GROUP, (i + 1) * GROUP):
                mark(c)

    pl.semaphore_wait(barrier, replicas - 1 + RING - 1)

    def owned(place):
        return lax.rem(place // RING, OWN) * OWN + lax.rem(place, OWN)

    def send_messages(peer):
        for i, (source, target) in enumerate(((sent_ids, recv_ids), (msg_ref, recv_values))):
            pltpu.make_async_remote_copy(
                src_ref=source.at[owned(peer)],
                dst_ref=target.at[me],
                send_sem=msg_send.at[i],
                recv_sem=msg_recv.at[i, z],
                device_id={"dp": peer},
                device_id_type=MESH,
            ).start()

    every_peer(send_messages)

    def paired(pieces):
        rows = []
        for piece in pieces:
            high, low = split(piece)
            for k in range(0, piece.shape[1], 128):
                rows.append(jnp.concatenate([high[:, k : k + 128], low[:, k : k + 128]], axis=1))
        both = dot(jnp.concatenate(rows, axis=0), inv_pair[...])
        both = both[:, :128] + both[:, 128:]
        return [both[k * BLOCK : (k + 1) * BLOCK] for k in range(len(rows))]

    small[3].wait()
    small[4].wait()
    mine = owned(me)
    recv_ids[me] = sent_ids[mine]
    recv_values[me] = msg_ref[mine]

    frequency = iota((BLOCK, 128), 0)
    lane_group = iota((RING, 128), 1) // TOPK
    own_group = lax.rem(iota((RING, 128), 0), 4) == lane_group

    def turns(rows):
        return [rows] + [pltpu.roll(rows, TOPK * k, 1) for k in range(1, 4)]

    def gathered(turned, k):
        out = turned[(-k) % 4]
        for g in range(1, 4):
            out = jnp.where(lane_group == g, turned[(g - k) % 4], out)
        out = jnp.where(own_group, out, jnp.zeros_like(out))
        out = out + pltpu.roll(out, 1, 0)
        return out + pltpu.roll(out, 2, 0)

    def combine(row, count):
        for i, ref in enumerate((recv_ids, recv_values)):
            arrived = ref.at[pl.ds(0, count)]
            pltpu.make_async_copy(arrived, arrived, msg_recv.at[i, row]).wait()
        flat_ids[...] = recv_ids[pl.ds(row * RING, RING)].reshape(2 * RING, 128)
        flat_values[...] = recv_values[pl.ds(row * RING, RING)].astype(F32).reshape(2 * RING, 128)
        for u in range(2):
            all_ids = turns(flat_ids[pl.ds(u, RING, stride=2), :])
            all_values = turns(flat_values[pl.ds(u, RING, stride=2), :])
            for k in range(4):
                ids, values = gathered(all_ids, k), gathered(all_values, k)
                ids_a, ids_b = ids // BLOCK, lax.rem(ids, BLOCK)
                rows, cols = [], []
                for j in (3, 7):
                    rows.append(jnp.where(frequency == ids_a[j : j + 1], values[j : j + 1], 0.0).astype(BF16))
                    cols.append(jnp.where(frequency == ids_b[j : j + 1], 1.0, 0.0).astype(BF16))
                part_ref[row, 4 * u + k] = dot_nt(jnp.concatenate(rows, axis=1), jnp.concatenate(cols, axis=1))

    combine(z, RING - 1)

    def combine_row(i, carry):
        combine(lax.rem(z + nearest(i) + RING, RING), RING)
        return carry

    lax.fori_loop(1, RING, combine_row, 0)

    def summed(k):
        total = part_ref[0, k]
        for row in range(1, RING):
            total = total + part_ref[row, k]
        return total

    combined = [jnp.concatenate([summed(k), summed(k + 1)], axis=1) for k in range(0, 8, 2)]
    energy = sum(jnp.sum(pair * pair, axis=0, keepdims=True) for pair in combined)

    def send_energy(ref, place, stage, targets):
        for target in targets:
            pltpu.make_async_remote_copy(
                src_ref=ref.at[place],
                dst_ref=ref.at[place],
                send_sem=e_send.at[stage],
                recv_sem=e_recv.at[stage],
                device_id=target,
                device_id_type=MESH,
            ).start()

    et_ref[tensor] = energy
    send_energy(et_ref, tensor, 0, [{"tensor": lax.rem(tensor + k, RING)} for k in (4, 5, 3, 2, 6, 7, 1)])

    halfway = paired(combined)
    quarter_rows = BLOCK // 4
    for k in range(2):
        decoded = left(inv_left[...], jnp.concatenate(halfway[2 * k : 2 * k + 2], axis=1))
        rounded = decoded.astype(BF16)
        for h in range(2):
            for part in range(2):
                start = (2 * h + part) * quarter_rows
                land_ref[h, mine, part, :, k * CHUNK : (k + 1) * CHUNK] = rounded[start : start + quarter_rows]

    along = ((y, z), (z, y))

    def place_of(h, a, b):
        a, b = lax.rem(a + RING, RING), lax.rem(b + RING, RING)
        return b * RING + a if h == 0 else a * RING + b

    def item_of(h, a, b):
        return owned(place_of(h, a, b))

    def send_item(h, ref, sem, target):
        pltpu.make_async_remote_copy(
            src_ref=ref,
            dst_ref=ref,
            send_sem=land_send.at[h],
            recv_sem=sem,
            device_id={"dp": target},
            device_id_type=MESH,
        ).start()

    def spread(h, turn, item, places):
        for side, place in enumerate(places[:2]):
            send_item(h, land_ref.at[h, item], land_recv.at[h, turn, side], place)
        for part, place in enumerate(places[2:]):
            send_item(h, land_ref.at[h, item, part], land_recv.at[h, turn, 2], place)

    def spread_first(h):
        a, b = along[h]
        spread(h, 0, mine, [place_of(h, a + step, b) for step in (1, -1, 2, -2)])

    def spread_second(h, item):
        a, b = along[h]
        spread(h, 1, item, [place_of(h, a, b + step) for step in (1, -1, 2, -2)])

    def wait_items(h, turn, side, count):
        ref = land_ref.at[h, pl.ds(0, count)]
        pltpu.make_async_copy(ref, ref, land_recv.at[h, turn, side]).wait()

    def take_energy(ref, stage, count):
        rest = ref.at[pl.ds(0, count - 1)]
        pltpu.make_async_copy(rest, rest, e_recv.at[stage]).wait()
        pltpu.make_async_copy(rest, rest, e_send.at[stage]).wait()
        row = ref[0]
        for k in range(1, count):
            row = row + ref[k]
        return row

    for h in range(2):
        spread_first(h)
    for h in range(2):
        spread_second(h, mine)
    for side, step in enumerate((-1, 1)):
        for h in range(2):
            a, b = along[h]
            wait_items(h, 0, side, 1)
            spread_second(h, item_of(h, a + step, b))
    ed_ref[mine] = take_energy(et_ref, 0, RING)
    near = [(i, j) for i in (-1, 0, 1, 2) for j in (-1, 0, 1, 2) if (i, j) != (0, 0)]
    send_energy(ed_ref, mine, 1, [{"dp": place_of(0, y + i, z + j)} for i, j in near])
    for h in range(2):
        a, b = along[h]
        wait_items(h, 0, 2, 1)
        spread_second(h, item_of(h, a + 2, b))

    def remove(i, carry):
        rows = []
        for c in range(GROUP):
            chunk = i * GROUP + c
            marker = dot_nt(oa_ref[chunk], ob_ref[chunk])
            rows.append(left(inv_left[...], spectrum_of(chunk) * marker))
        restored = paired(rows)
        for c in range(GROUP):
            chunk = i * GROUP + c
            columns = pl.ds(pl.multiple_of(chunk * CHUNK, CHUNK), CHUNK)
            taken = jnp.concatenate(restored[2 * c : 2 * c + 2], axis=1)
            nm_ref[:, columns] = (renewed(chunk) - taken).astype(BF16)
        return carry

    lax.fori_loop(0, groups, remove, 0)

    energy = jnp.sum(take_energy(ed_ref, 1, OWN * OWN), axis=1, keepdims=True)
    scale = 1.0 / jnp.sqrt(energy / total_count + EPSILON)

    def finish(h, item):
        columns = pl.ds(pl.multiple_of(item * 2 * CHUNK, 2 * CHUNK), 2 * CHUNK)
        for part in range(2):
            start = (2 * h + part) * quarter_rows
            up_ref[start : start + quarter_rows, columns] = (
                land_ref[h, item, part].astype(F32) * scale
            ).astype(BF16)

    for side, other in ((None, 0), (0, -1), (1, 1), (2, 2)):
        for h in range(2):
            a, b = along[h]
            if side is not None:
                wait_items(h, 1, side, OWN)
            for step in (0, 1, -1, 2):
                finish(h, item_of(h, a + step, b + other))

    for i, ref in enumerate((recv_ids, recv_values)):
        others = ref.at[pl.ds(0, replicas - 1)]
        pltpu.make_async_copy(others, others, msg_send.at[i]).wait()
    for h in range(2):
        rest = land_ref.at[h, pl.ds(0, OWN * OWN - 1)]
        pltpu.make_async_copy(rest, rest, land_send.at[h]).wait()


def deliver(nm_ref, up_ref, nm_hbm, up_hbm, sem):
    copies = [
        pltpu.make_async_copy(nm_ref, nm_hbm.at[0], sem.at[0]),
        pltpu.make_async_copy(up_ref, up_hbm, sem.at[1]),
    ]
    for copy in copies:
        copy.start()
    for copy in copies:
        copy.wait()


def local(total_count, gradient, momentum, indices):
    _, height, columns = gradient.shape
    chunks = columns // CHUNK
    groups = chunks // GROUP
    replicas = RING * RING
    cosines = basis()
    anywhere = pl.BlockSpec(memory_space=pl.ANY)
    dma = pltpu.SemaphoreType.DMA
    nm, up = pl.pallas_call(
        functools.partial(kernel, total_count),
        out_shape=(
            pltpu.VMEM((height, columns), BF16),
            pltpu.VMEM((height, columns), BF16),
        ),
        in_specs=[anywhere] * 7,
        out_specs=(pl.BlockSpec(memory_space=pltpu.VMEM),) * 2,
        scratch_shapes=[
            pltpu.VMEM((TOPK, columns // BLOCK), jnp.int32),
            pltpu.VMEM((256, 256), BF16),
            pltpu.VMEM((256, 256), BF16),
            pltpu.VMEM((128, 128), BF16),
            pltpu.VMEM((BLOCK, 256), BF16),
            pltpu.VMEM((height, columns), BF16),
            pltpu.VMEM((height, columns), BF16),
            pltpu.VMEM((chunks * 2 * BLOCK, 256), BF16),
            pltpu.VMEM((chunks * 2 * BLOCK, 128), F32),
            pltpu.VMEM((chunks, CHUNK, 128), BF16),
            pltpu.VMEM((chunks, BLOCK, 128), BF16),
            pltpu.VMEM((chunks * 4, TOPK), jnp.int32),
            pltpu.VMEM((chunks, 128), jnp.int32),
            pltpu.VMEM((OWN * OWN, 2, 128), jnp.int32),
            pltpu.VMEM((OWN * OWN, 2, 128), BF16),
            pltpu.VMEM((replicas, 2, 128), jnp.int32),
            pltpu.VMEM((replicas, 2, 128), BF16),
            pltpu.VMEM((2 * RING, 128), jnp.int32),
            pltpu.VMEM((2 * RING, 128), F32),
            pltpu.VMEM((RING, 8, BLOCK, BLOCK), F32),
            pltpu.VMEM((2, OWN * OWN, 2, BLOCK // 4, 2 * CHUNK), BF16),
            pltpu.VMEM((RING, 1, 128), F32),
            pltpu.VMEM((OWN * OWN, 1, 128), F32),
            dma((5,)),
            dma((2, groups)),
            dma((2,)),
            dma((2, RING)),
            dma((2,)),
            dma((2, 2, 3)),
            dma((2,)),
            dma((2,)),
        ],
        compiler_params=pltpu.CompilerParams(collective_id=0, has_side_effects=True, vmem_limit_bytes=64880640),
        name="demo_step",
    )(
        gradient,
        momentum,
        jnp.transpose(indices.reshape(columns // BLOCK, TOPK)),
        pair_constants(cosines.T),
        pair_constants(cosines),
        entry_constants(cosines),
        left_constants(cosines.T),
    )
    return pl.pallas_call(
        deliver,
        out_shape=(
            jax.ShapeDtypeStruct((1, height, columns), BF16),
            jax.ShapeDtypeStruct((height, columns), BF16),
        ),
        in_specs=[pl.BlockSpec(memory_space=pltpu.VMEM)] * 2,
        out_specs=(anywhere, anywhere),
        scratch_shapes=[dma((2,))],
        compiler_params=pltpu.CompilerParams(vmem_limit_bytes=2**20),
        name="deliver",
    )(nm, up)


def solution(mesh):
    def whole(gradient, momentum, indices):
        rows, columns = gradient.shape[1:]
        return jax.shard_map(
            functools.partial(local, float(rows * columns)),
            mesh=mesh,
            in_specs=(P("dp", "tensor", None), P("dp", "tensor", None), P("dp", "tensor", None, None)),
            out_specs=(P("dp", "tensor", None), P("tensor", None)),
            check_vma=False,
        )(gradient, momentum, indices)

    return whole
```

```python
import functools

import jax
import jax.numpy as jnp
import numpy as np
from jax import lax
from jax.experimental import pallas as pl
from jax.experimental.pallas import tpu as pltpu
from jax.sharding import PartitionSpec as P

MESH = pl.DeviceIdType.MESH
BLOCK = 64
TOPK = 32
CHUNK = 256
RING = 8
OWN = 4
GROUP = 32
EPSILON = 1e-06
DECAY = 0.999
F32 = jnp.float32
BF16 = jnp.bfloat16


def basis():
    frequency = np.arange(BLOCK, dtype=np.float64)[:, None]
    position = np.arange(BLOCK, dtype=np.float64)[None, :]
    waves = np.cos(np.pi * (2.0 * position + 1.0) * frequency / (2.0 * BLOCK))
    return waves * np.where(frequency == 0.0, np.sqrt(1.0 / BLOCK), np.sqrt(2.0 / BLOCK))


def halves(array):
    array = array.astype(np.float32)
    high = array.astype(BF16)
    low = (array - high.astype(np.float32)).astype(BF16)
    return high, low


def pair_constants(matrix):
    pair = np.concatenate([np.kron(np.eye(2), half.astype(np.float32)).astype(BF16) for half in halves(matrix)], axis=1)
    return np.concatenate([pair, pair], axis=0)


def entry_constants(matrix):
    return np.concatenate(
        [np.concatenate(pair, axis=1) for pair in zip(halves(DECAY * matrix), halves(matrix))], axis=0
    )


def left_constants(matrix):
    high, low = halves(matrix)
    return np.concatenate([high, high, low, low], axis=1)


def dot(a, b):
    return jnp.dot(a, b, preferred_element_type=F32)


def dot_nt(a, b):
    return lax.dot_general(a, b, (((1,), (1,)), ((), ())), preferred_element_type=F32)


def split(x):
    high = x.astype(BF16)
    return high, (x - high.astype(F32)).astype(BF16)


def left(constants, y):
    high, low = split(y)
    return dot(constants, jnp.concatenate([high, low, high, low], axis=0))


def iota(shape, dim):
    return lax.broadcasted_iota(jnp.int32, shape, dim)


def kernel(
    total_count,
    g_hbm,
    m_hbm,
    idx_hbm,
    fwd_pair_hbm,
    inv_pair_hbm,
    entry_hbm,
    inv_left_hbm,
    nm_ref,
    up_ref,
    idx_ref,
    fwd_pair,
    inv_pair,
    entry,
    inv_left,
    g_ref,
    m_ref,
    y_ref,
    s_ref,
    ob_ref,
    oa_ref,
    turned_ref,
    il_ref,
    sent_ids,
    msg_ref,
    recv_ids,
    recv_values,
    flat_ids,
    flat_values,
    part_ref,
    land_ref,
    et_ref,
    ed_ref,
    const_sem,
    in_sem,
    msg_send,
    msg_recv,
    land_send,
    land_recv,
    e_send,
    e_recv,
):
    me = lax.axis_index("dp")
    tensor = lax.axis_index("tensor")
    z, y = me // RING, lax.rem(me, RING)
    replicas = RING * RING
    chunks = ob_ref.shape[0]
    groups = chunks // GROUP
    wide = GROUP * CHUNK

    def group_columns(i):
        return pl.ds(pl.multiple_of(i * wide, wide), wide)

    def load(i, which):
        hbm, ref = ((g_hbm, g_ref), (m_hbm, m_ref))[which]
        return pltpu.make_async_copy(
            hbm.at[0, :, group_columns(i)], ref.at[:, group_columns(i)], in_sem.at[which, i]
        )

    small = [
        pltpu.make_async_copy(hbm, ref, const_sem.at[i])
        for i, (hbm, ref) in enumerate(
            [
                (idx_hbm, idx_ref),
                (entry_hbm, entry),
                (fwd_pair_hbm, fwd_pair),
                (inv_pair_hbm, inv_pair),
                (inv_left_hbm, inv_left),
            ]
        )
    ]
    for copy in small[:3]:
        copy.start()
    for i in range(groups):
        load(i, 0).start()
        load(i, 1).start()
    for copy in small[3:]:
        copy.start()

    barrier = pltpu.get_barrier_semaphore()

    def nearest(i):
        return ((i + 1) // 2) * (2 * lax.rem(i, 2) - 1)

    def far_first(i, visit, own):
        peer_z = lax.rem(z + nearest(RING - 1 - i) + RING, RING)
        for step in (4, 3, -3, 2, -2, 1, -1):
            visit(peer_z * RING + lax.rem(y + step + RING, RING))
        if not own:
            visit(peer_z * RING + y)

    def every_peer(visit):
        def row(i, carry):
            far_first(i, visit, False)
            return carry

        lax.fori_loop(0, RING - 1, row, 0)
        far_first(RING - 1, visit, True)

    def greet(peer):
        pl.semaphore_signal(barrier, inc=1, device_id={"dp": peer}, device_id_type=MESH)

    def greet_tensor(k, carry):
        pl.semaphore_signal(barrier, inc=1, device_id={"tensor": lax.rem(tensor + k, RING)}, device_id_type=MESH)
        return carry

    every_peer(greet)
    lax.fori_loop(1, RING, greet_tensor, 0)

    small[0].wait()
    turned_ref[...] = jnp.transpose(idx_ref[...])
    il_ref[...] = jnp.concatenate(
        [turned_ref[pl.ds(k, chunks, stride=4), :] for k in range(4)], axis=1
    )
    lane_span = iota((1, 128), 1) // TOPK

    def mark(chunk):
        ids = il_ref[chunk : chunk + 1, :]
        row_hit = iota((BLOCK, 128), 0) == ids // BLOCK
        col_hit = iota((CHUNK, 128), 0) == lax.rem(ids, BLOCK) + BLOCK * lane_span
        ob_ref[chunk] = jnp.where(col_hit, 1.0, 0.0).astype(BF16)
        oa_ref[chunk] = jnp.where(row_hit, 1.0, 0.0).astype(BF16)
        sent_ids[chunk // 2, chunk % 2 : chunk % 2 + 1, :] = ids

    def renewed(c):
        columns = pl.ds(pl.multiple_of(c * CHUNK, CHUNK), CHUNK)
        return DECAY * m_ref[:, columns].astype(F32) + g_ref[:, columns].astype(F32)

    small[1].wait()
    small[2].wait()

    def rows_first(i):
        load(i, 0).wait()
        load(i, 1).wait()
        for c in range(i * GROUP, (i + 1) * GROUP):
            columns = slice(c * CHUNK, (c + 1) * CHUNK)
            both = dot(entry[...], jnp.concatenate([m_ref[:, columns], g_ref[:, columns]], axis=0))
            high, low = split(both[:BLOCK] + both[BLOCK:])
            for k in range(2):
                rows = slice((2 * c + k) * BLOCK, (2 * c + k + 1) * BLOCK)
                y_ref[rows, :128] = high[:, k * 128 : (k + 1) * 128]
                y_ref[rows, 128:] = low[:, k * 128 : (k + 1) * 128]

    def columns_next(i):
        rows = slice(i * GROUP * 2 * BLOCK, (i + 1) * GROUP * 2 * BLOCK)
        both = dot(y_ref[rows, :], fwd_pair[...])
        s_ref[rows, :] = both[:, :128] + both[:, 128:]

    def spectrum_of(c):
        start = c * 2 * BLOCK
        return jnp.concatenate([s_ref[pl.ds(start, BLOCK), :], s_ref[pl.ds(start + BLOCK, BLOCK), :]], axis=1)

    def pick(i):
        for c in range(i * GROUP, (i + 1) * GROUP):
            by_column = dot(spectrum_of(c).astype(BF16), ob_ref[c])
            row = jnp.sum(by_column * oa_ref[c].astype(F32), axis=0, keepdims=True)
            if c % 2:
                msg_ref[c // 2] = jnp.concatenate([before, row], axis=0).astype(BF16)
            before = row

    for i in range(groups + 2):
        if i >= 2:
            pick(i - 2)
        if 1 <= i <= groups:
            columns_next(i - 1)
        if i < groups:
            rows_first(i)
            for c in range(i * GROUP, (i + 1) * GROUP):
                mark(c)

    pl.semaphore_wait(barrier, replicas - 1 + RING - 1)

    def owned(place):
        return lax.rem(place // RING, OWN) * OWN + lax.rem(place, OWN)

    def send_messages(peer):
        for i, (source, target) in enumerate(((sent_ids, recv_ids), (msg_ref, recv_values))):
            pltpu.make_async_remote_copy(
                src_ref=source.at[owned(peer)],
                dst_ref=target.at[me],
                send_sem=msg_send.at[i],
                recv_sem=msg_recv.at[i, z],
                device_id={"dp": peer},
                device_id_type=MESH,
            ).start()

    every_peer(send_messages)

    def paired(pieces):
        rows = []
        for piece in pieces:
            high, low = split(piece)
            for k in range(0, piece.shape[1], 128):
                rows.append(jnp.concatenate([high[:, k : k + 128], low[:, k : k + 128]], axis=1))
        both = dot(jnp.concatenate(rows, axis=0), inv_pair[...])
        both = both[:, :128] + both[:, 128:]
        return [both[k * BLOCK : (k + 1) * BLOCK] for k in range(len(rows))]

    small[3].wait()
    small[4].wait()
    mine = owned(me)
    recv_ids[me] = sent_ids[mine]
    recv_values[me] = msg_ref[mine]

    frequency = iota((BLOCK, 128), 0)
    lane_group = iota((RING, 128), 1) // TOPK
    own_group = lax.rem(iota((RING, 128), 0), 4) == lane_group

    def turns(rows):
        return [rows] + [pltpu.roll(rows, TOPK * k, 1) for k in range(1, 4)]

    def gathered(turned, k):
        out = turned[(-k) % 4]
        for g in range(1, 4):
            out = jnp.where(lane_group == g, turned[(g - k) % 4], out)
        out = jnp.where(own_group, out, jnp.zeros_like(out))
        out = out + pltpu.roll(out, 1, 0)
        return out + pltpu.roll(out, 2, 0)

    def arrive(row, count):
        for i, ref in enumerate((recv_ids, recv_values)):
            arrived = ref.at[pl.ds(0, count)]
            pltpu.make_async_copy(arrived, arrived, msg_recv.at[i, row]).wait()

    def combine(row, slot):
        flat_ids[slot] = recv_ids[pl.ds(row * RING, RING)].reshape(2 * RING, 128)
        flat_values[slot] = recv_values[pl.ds(row * RING, RING)].astype(F32).reshape(2 * RING, 128)
        for u in range(2):
            all_ids = turns(flat_ids[slot, pl.ds(u, RING, stride=2), :])
            all_values = turns(flat_values[slot, pl.ds(u, RING, stride=2), :])
            for k in range(4):
                ids, values = gathered(all_ids, k), gathered(all_values, k)
                ids_a, ids_b = ids // BLOCK, lax.rem(ids, BLOCK)
                rows, cols = [], []
                for j in (3, 7):
                    rows.append(jnp.where(frequency == ids_a[j : j + 1], values[j : j + 1], 0.0).astype(BF16))
                    cols.append(jnp.where(frequency == ids_b[j : j + 1], 1.0, 0.0).astype(BF16))
                part_ref[row, 4 * u + k] = dot_nt(jnp.concatenate(rows, axis=1), jnp.concatenate(cols, axis=1))

    arrive(z, RING - 1)
    combine(z, 0)

    def combine_pair(k, carry):
        pair = (lax.rem(z + k, RING), lax.rem(z + RING - k, RING))
        for row in pair:
            arrive(row, RING)
        for slot, row in enumerate(pair):
            combine(row, slot)
        return carry

    lax.fori_loop(1, RING // 2, combine_pair, 0)
    arrive(lax.rem(z + RING // 2, RING), RING)
    combine(lax.rem(z + RING // 2, RING), 0)

    def summed(k):
        total = part_ref[0, k]
        for row in range(1, RING):
            total = total + part_ref[row, k]
        return total

    combined = [jnp.concatenate([summed(k), summed(k + 1)], axis=1) for k in range(0, 8, 2)]
    energy = sum(jnp.sum(pair * pair, axis=0, keepdims=True) for pair in combined)

    def send_energy(ref, place, stage, targets):
        for target in targets:
            pltpu.make_async_remote_copy(
                src_ref=ref.at[place],
                dst_ref=ref.at[place],
                send_sem=e_send.at[stage],
                recv_sem=e_recv.at[stage],
                device_id=target,
                device_id_type=MESH,
            ).start()

    et_ref[tensor] = energy
    send_energy(et_ref, tensor, 0, [{"tensor": lax.rem(tensor + k, RING)} for k in (4, 5, 3, 2, 6, 7, 1)])

    halfway = paired(combined)
    quarter_rows = BLOCK // 4
    for k in range(2):
        decoded = left(inv_left[...], jnp.concatenate(halfway[2 * k : 2 * k + 2], axis=1))
        rounded = decoded.astype(BF16)
        for h in range(2):
            for part in range(2):
                start = (2 * h + part) * quarter_rows
                land_ref[h, mine, part, :, k * CHUNK : (k + 1) * CHUNK] = rounded[start : start + quarter_rows]

    along = ((y, z), (z, y))

    def place_of(h, a, b):
        a, b = lax.rem(a + RING, RING), lax.rem(b + RING, RING)
        return b * RING + a if h == 0 else a * RING + b

    def item_of(h, a, b):
        return owned(place_of(h, a, b))

    def send_item(h, ref, sem, target):
        pltpu.make_async_remote_copy(
            src_ref=ref,
            dst_ref=ref,
            send_sem=land_send.at[h],
            recv_sem=sem,
            device_id={"dp": target},
            device_id_type=MESH,
        ).start()

    def spread(h, turn, item, places):
        for side, place in enumerate(places[:2]):
            send_item(h, land_ref.at[h, item], land_recv.at[h, turn, side], place)
        for part, place in enumerate(places[2:]):
            send_item(h, land_ref.at[h, item, part], land_recv.at[h, turn, 2], place)

    def spread_first(h):
        a, b = along[h]
        spread(h, 0, mine, [place_of(h, a + step, b) for step in (1, -1, 2, -2)])

    def spread_second(h, item):
        a, b = along[h]
        spread(h, 1, item, [place_of(h, a, b + step) for step in (1, -1, 2, -2)])

    def wait_items(h, turn, side, count):
        ref = land_ref.at[h, pl.ds(0, count)]
        pltpu.make_async_copy(ref, ref, land_recv.at[h, turn, side]).wait()

    def take_energy(ref, stage, count):
        rest = ref.at[pl.ds(0, count - 1)]
        pltpu.make_async_copy(rest, rest, e_recv.at[stage]).wait()
        pltpu.make_async_copy(rest, rest, e_send.at[stage]).wait()
        row = ref[0]
        for k in range(1, count):
            row = row + ref[k]
        return row

    for h in range(2):
        spread_first(h)
    for h in range(2):
        spread_second(h, mine)
    for side, step in enumerate((-1, 1)):
        for h in range(2):
            a, b = along[h]
            wait_items(h, 0, side, 1)
            spread_second(h, item_of(h, a + step, b))
    for h in range(2):
        a, b = along[h]
        wait_items(h, 0, 2, 1)
        spread_second(h, item_of(h, a + 2, b))
    ed_ref[mine] = take_energy(et_ref, 0, RING)
    near = [(i, j) for i in (-1, 0, 1, 2) for j in (-1, 0, 1, 2) if (i, j) != (0, 0)]
    send_energy(ed_ref, mine, 1, [{"dp": place_of(0, y + i, z + j)} for i, j in near])

    def remove(i, carry):
        rows = []
        for c in range(GROUP // 2):
            chunk = i * (GROUP // 2) + c
            marker = dot_nt(oa_ref[chunk], ob_ref[chunk])
            rows.append(left(inv_left[...], spectrum_of(chunk) * marker))
        restored = paired(rows)
        for c in range(GROUP // 2):
            chunk = i * (GROUP // 2) + c
            columns = pl.ds(pl.multiple_of(chunk * CHUNK, CHUNK), CHUNK)
            taken = jnp.concatenate(restored[2 * c : 2 * c + 2], axis=1)
            nm_ref[:, columns] = (renewed(chunk) - taken).astype(BF16)
        return carry

    lax.fori_loop(0, 2 * groups, remove, 0)

    energy = jnp.sum(take_energy(ed_ref, 1, OWN * OWN), axis=1, keepdims=True)
    scale = 1.0 / jnp.sqrt(energy / total_count + EPSILON)

    def finish(h, item):
        columns = pl.ds(pl.multiple_of(item * 2 * CHUNK, 2 * CHUNK), 2 * CHUNK)
        for part in range(2):
            start = (2 * h + part) * quarter_rows
            up_ref[start : start + quarter_rows, columns] = (
                land_ref[h, item, part].astype(F32) * scale
            ).astype(BF16)

    for side, other in ((None, 0), (0, -1), (1, 1), (2, 2)):
        for h in range(2):
            a, b = along[h]
            if side is not None:
                wait_items(h, 1, side, OWN)
            for step in (0, 1, -1, 2):
                finish(h, item_of(h, a + step, b + other))

    for i, ref in enumerate((recv_ids, recv_values)):
        others = ref.at[pl.ds(0, replicas - 1)]
        pltpu.make_async_copy(others, others, msg_send.at[i]).wait()
    for h in range(2):
        rest = land_ref.at[h, pl.ds(0, OWN * OWN - 1)]
        pltpu.make_async_copy(rest, rest, land_send.at[h]).wait()


def deliver(nm_ref, up_ref, nm_hbm, up_hbm, sem):
    copies = [
        pltpu.make_async_copy(nm_ref, nm_hbm.at[0], sem.at[0]),
        pltpu.make_async_copy(up_ref, up_hbm, sem.at[1]),
    ]
    for copy in copies:
        copy.start()
    for copy in copies:
        copy.wait()


def local(total_count, gradient, momentum, indices):
    _, height, columns = gradient.shape
    chunks = columns // CHUNK
    groups = chunks // GROUP
    replicas = RING * RING
    cosines = basis()
    anywhere = pl.BlockSpec(memory_space=pl.ANY)
    dma = pltpu.SemaphoreType.DMA
    nm, up = pl.pallas_call(
        functools.partial(kernel, total_count),
        out_shape=(
            pltpu.VMEM((height, columns), BF16),
            pltpu.VMEM((height, columns), BF16),
        ),
        in_specs=[anywhere] * 7,
        out_specs=(pl.BlockSpec(memory_space=pltpu.VMEM),) * 2,
        scratch_shapes=[
            pltpu.VMEM((TOPK, columns // BLOCK), jnp.int32),
            pltpu.VMEM((256, 256), BF16),
            pltpu.VMEM((256, 256), BF16),
            pltpu.VMEM((128, 128), BF16),
            pltpu.VMEM((BLOCK, 256), BF16),
            pltpu.VMEM((height, columns), BF16),
            pltpu.VMEM((height, columns), BF16),
            pltpu.VMEM((chunks * 2 * BLOCK, 256), BF16),
            pltpu.VMEM((chunks * 2 * BLOCK, 128), F32),
            pltpu.VMEM((chunks, CHUNK, 128), BF16),
            pltpu.VMEM((chunks, BLOCK, 128), BF16),
            pltpu.VMEM((chunks * 4, TOPK), jnp.int32),
            pltpu.VMEM((chunks, 128), jnp.int32),
            pltpu.VMEM((OWN * OWN, 2, 128), jnp.int32),
            pltpu.VMEM((OWN * OWN, 2, 128), BF16),
            pltpu.VMEM((replicas, 2, 128), jnp.int32),
            pltpu.VMEM((replicas, 2, 128), BF16),
            pltpu.VMEM((2, 2 * RING, 128), jnp.int32),
            pltpu.VMEM((2, 2 * RING, 128), F32),
            pltpu.VMEM((RING, 8, BLOCK, BLOCK), F32),
            pltpu.VMEM((2, OWN * OWN, 2, BLOCK // 4, 2 * CHUNK), BF16),
            pltpu.VMEM((RING, 1, 128), F32),
            pltpu.VMEM((OWN * OWN, 1, 128), F32),
            dma((5,)),
            dma((2, groups)),
            dma((2,)),
            dma((2, RING)),
            dma((2,)),
            dma((2, 2, 3)),
            dma((2,)),
            dma((2,)),
        ],
        compiler_params=pltpu.CompilerParams(collective_id=0, has_side_effects=True, vmem_limit_bytes=64880640),
        name="demo_step",
    )(
        gradient,
        momentum,
        jnp.transpose(indices.reshape(columns // BLOCK, TOPK)),
        pair_constants(cosines.T),
        pair_constants(cosines),
        entry_constants(cosines),
        left_constants(cosines.T),
    )
    return pl.pallas_call(
        deliver,
        out_shape=(
            jax.ShapeDtypeStruct((1, height, columns), BF16),
            jax.ShapeDtypeStruct((height, columns), BF16),
        ),
        in_specs=[pl.BlockSpec(memory_space=pltpu.VMEM)] * 2,
        out_specs=(anywhere, anywhere),
        scratch_shapes=[dma((2,))],
        compiler_params=pltpu.CompilerParams(vmem_limit_bytes=2**20),
        name="deliver",
    )(nm, up)


def solution(mesh):
    def whole(gradient, momentum, indices):
        rows, columns = gradient.shape[1:]
        return jax.shard_map(
            functools.partial(local, float(rows * columns)),
            mesh=mesh,
            in_specs=(P("dp", "tensor", None), P("dp", "tensor", None), P("dp", "tensor", None, None)),
            out_specs=(P("dp", "tensor", None), P("tensor", None)),
            check_vma=False,
        )(gradient, momentum, indices)

    return whole
```
